128 devices in a mesh: samp: 2 (over core), grid: 64 (over z, y, x).
Axes of the slice: x: 4, y: 4, z: 4, core: 2. Of those that a mesh axis runs over, the one named last changes fastest.
Arguments:
- log_coef: float32 [2, 4096, 2048], P('samp', 'grid'), may hold values from -4 to 4
- source: float32 [2, 4096, 2048], P('samp', 'grid'), may hold values from -0.6 to 0.6
Outputs:
- correction: float32 [2, 4096, 2048], P('samp', 'grid')
- level_mean: float32 [4096, 2048], P('grid', 'samp')
- level_var: float32 [4096, 2048], P('grid', 'samp')
The draws below stay inside these ranges and needn't reach their ends.
All inputs are finite; a program needn't handle non-finite values.
Results may differ from the reference program's by a relative error of at most 0.0003.
Values sent between devices are 32-bit elements; how exact they have to be, the bound alone decides.
No kernel may reach another device: no remote copies, remote signals or barrier semaphores. Data moves between devices by JAX's collectives and lax.ppermute only.
A program may use at most 192 MiB of HBM per device.

```python
import jax
import jax.numpy as jnp
from jax import lax

NY = 2048
LEVELS = 5
VCYCLES = 2
COARSE_SWEEPS = 4
NX = 4096
SAMPLES = 2


def level_of(stream_key, dims, shards, smallest, largest):
    factor_of, own = 1.0, jax.random.fold_in(stream_key, 6)
    for axis_at, parts in shards:
        heights = jnp.exp(jax.random.uniform(jax.random.fold_in(own, axis_at), (parts,), jnp.float32, smallest / len(shards), largest / len(shards)))
        factor_of = factor_of * jnp.repeat(heights, dims[axis_at] // parts).reshape([-1 if axis == axis_at else 1 for axis in range(len(dims))])
    return factor_of


def bell_draw(rng, extent, deviation, bound, pieces=(), held_as=jnp.bfloat16):
    loudness = level_of(rng, extent, pieces, -0.22, 0.18) if pieces else 1.0
    array = jax.random.normal(rng, extent, jnp.float32) * deviation * loudness
    return jnp.minimum(jnp.maximum(array, -bound), bound).astype(held_as)


def setup_inputs(seed: int = 0) -> dict:
    key_of = jax.random.split(jax.random.key(seed), 3)
    return {
        "log_coef": bell_draw(key_of[0], (SAMPLES, NX, NY), 1.0, 4.0, ((0, 2), (1, 64)), jnp.float32),
        "source": bell_draw(key_of[1], (SAMPLES, NX, NY), 0.1, 0.6, ((0, 2), (1, 64)), jnp.float32),
    }


damping = 0.8


def harmonic(former, latter):
    return 2.0 * former * latter / (former + latter)


def halve(coeffs):
    row_count, col_count = coeffs.shape
    return jnp.mean(coeffs.reshape(row_count // 2, 2, col_count // 2, 2), axis=(1, 3))


def quad_sum(values):
    row_count, col_count = values.shape
    return jnp.sum(values.reshape(row_count // 2, 2, col_count // 2, 2), axis=(1, 3))


def expand(values):
    return jnp.repeat(jnp.repeat(values, 2, axis=0), 2, axis=1)


def side_weights(coeffs):
    shifted = jnp.concatenate([coeffs[:, 1:], coeffs[:, -1:]], axis=1)
    east_face = harmonic(coeffs, shifted)
    west_face = jnp.concatenate([harmonic(coeffs[:, :1], coeffs[:, :1]), east_face[:, :-1]], axis=1)
    return west_face, east_face


def level_weights(coeffs):
    west_face, east_face = side_weights(coeffs)
    padded = jnp.concatenate([coeffs[:1], coeffs, coeffs[-1:]], axis=0)
    return west_face, east_face, harmonic(padded[:-1], padded[1:])


def pad_rows(values):
    return jnp.pad(values, ((1, 1), (0, 0)))


def apply_rows(wide, west_face, east_face, vertical):
    middle = wide[1:-1]
    zero_column = jnp.zeros_like(middle[:, :1])
    west_values = jnp.concatenate([zero_column, middle[:, :-1]], axis=1)
    east_values = jnp.concatenate([middle[:, 1:], zero_column], axis=1)
    north_face = vertical[:-1]
    south_face = vertical[1:]
    diagonal = west_face + east_face + north_face + south_face
    applied = diagonal * middle - (west_face * west_values + east_face * east_values
                                   + north_face * wide[:-2] + south_face * wide[2:])
    return middle, applied, diagonal


def relax_rows(wide, right_side, west_face, east_face, vertical):
    middle, applied, diagonal = apply_rows(wide, west_face, east_face, vertical)
    return middle + damping * (right_side - applied) / diagonal


def vcycle(height, iterate, right_side, ladder):
    weights = ladder[height]
    if height == len(ladder) - 1:
        for repeat in range(COARSE_SWEEPS):
            iterate = relax_rows(pad_rows(iterate), right_side, *weights)
        return iterate
    for repeat in range(2):
        iterate = relax_rows(pad_rows(iterate), right_side, *weights)
    middle, applied, diagonal = apply_rows(pad_rows(iterate), *weights)
    coarse_side = quad_sum(right_side - applied)
    errors = vcycle(height + 1, jnp.zeros_like(coarse_side), coarse_side, ladder)
    iterate = iterate + expand(errors)
    for repeat in range(2):
        iterate = relax_rows(pad_rows(iterate), right_side, *weights)
    return iterate


def one_sample(sample_pair):
    log_field, source_field = sample_pair
    coeffs = jnp.exp(log_field)
    ladder = []
    for height in range(LEVELS):
        if height:
            coeffs = halve(coeffs)
        ladder.append(level_weights(coeffs))
    fine_field = jnp.zeros_like(source_field)
    for repeat in range(VCYCLES):
        fine_field = vcycle(0, fine_field, source_field, ladder)
    coarse_side = quad_sum(source_field)
    coarse = jnp.zeros_like(coarse_side)
    for repeat in range(VCYCLES):
        coarse = vcycle(1, coarse, coarse_side, ladder)
    return fine_field - expand(coarse)


def reference(log_coef, source):
    correction = lax.map(one_sample, (log_coef, source))
    summed = jnp.sum(correction, axis=0)
    squares = jnp.sum(correction * correction, axis=0)
    level_mean = summed / SAMPLES
    level_var = (squares - SAMPLES * level_mean * level_mean) / (SAMPLES - 1)
    return correction, level_mean, level_var
```

```python
import functools

import jax
import jax.numpy as jnp
from jax import lax
from jax.experimental import pallas as pl
from jax.experimental.pallas import tpu as pltpu
from jax.sharding import PartitionSpec as P

LANES = 128
PAD = 8
OWN = (64, 32, 16, 8, 4)
HALO = (24, 12, 32, 16, 8)
ROWS = tuple(o + 2 * h for o, h in zip(OWN, HALO))
TILES = (16, 8, 4, 2, 1)
STRIPS = (14, 7, 10, 5, 3)
BUF = tuple(8 * s + 2 * PAD for s in STRIPS)
DAMP = 0.8
F32 = jnp.float32


def loop(count, body, unroll=1):
    lax.fori_loop(0, count, lambda i, c: (body(i), c)[1], 0, unroll=unroll)


def at(i, offset):
    return pl.ds(pl.multiple_of(i * 8, 8) + offset, 8)


def lane_of(x):
    return lax.broadcasted_iota(jnp.int32, x.shape, 2)


def side_values(x):
    lane = lane_of(x)
    right = pltpu.roll(x, 1, 2)
    left = pltpu.roll(x, LANES - 1, 2)
    if x.shape[0] > 1:
        before = jnp.concatenate([right[-1:], right[:-1]], axis=0)
        after = jnp.concatenate([left[1:], left[:1]], axis=0)
        right = jnp.where(lane == 0, before, right)
        left = jnp.where(lane == LANES - 1, after, left)
    return right, left


def harmonic(a, b):
    return 2.0 * a * b / (a + b)


def make_weights(level, c_ref, a_ref, first_row, total_rows):
    def body(i):
        c = c_ref[:, at(i, PAD), :]
        north = c_ref[:, at(i, PAD - 1), :]
        south = c_ref[:, at(i, PAD + 1), :]
        west, east = side_values(c)
        tile = lax.broadcasted_iota(jnp.int32, c.shape, 0)
        lane = lane_of(c)
        row = first_row + i * 8 + lax.broadcasted_iota(jnp.int32, c.shape, 1)
        at_west = jnp.logical_and(tile == 0, lane == 0)
        at_east = jnp.logical_and(tile == c.shape[0] - 1, lane == LANES - 1)
        inside = jnp.logical_and(row >= 0, row < total_rows)
        w_west = harmonic(c, jnp.where(at_west, c, west))
        w_east = harmonic(c, jnp.where(at_east, c, east))
        w_north = harmonic(c, jnp.where(row == 0, c, north))
        w_south = harmonic(c, jnp.where(row == total_rows - 1, c, south))
        diagonal = w_west + w_east + w_north + w_south
        gain = jnp.where(inside, DAMP / diagonal, 0.0)
        rows = at(i, 0)
        a_ref[0, :, rows, :] = jnp.where(at_west, 0.0, gain * w_west)
        a_ref[1, :, rows, :] = jnp.where(at_east, 0.0, gain * w_east)
        a_ref[2, :, rows, :] = gain * w_north
        a_ref[3, :, rows, :] = gain * w_south
        a_ref[4, :, rows, :] = gain
        a_ref[5, :, rows, :] = diagonal * (1.0 / DAMP)

    loop(STRIPS[level], body)


def change(i, v_ref, b_ref, a_ref, start, count):
    tiles = pl.ds(start, count)
    v = v_ref[tiles, at(i, PAD), :]
    north = v_ref[tiles, at(i, PAD - 1), :]
    south = v_ref[tiles, at(i, PAD + 1), :]
    west, east = side_values(v)
    rows = at(i, 0)
    moved = a_ref[0, :, rows, :] * west + a_ref[1, :, rows, :] * east
    moved += a_ref[2, :, rows, :] * north + a_ref[3, :, rows, :] * south
    return v, moved + b_ref[tiles, at(i, PAD), :]


def solves(level, v_ref):
    tiles = TILES[level]
    return [(s, tiles) for s in range(0, v_ref.shape[0], tiles)]


def relax(level, v_ref, out_ref, b_ref, a_ref):
    def body(i):
        for start, count in solves(level, v_ref):
            v, moved = change(i, v_ref, b_ref, a_ref, start, count)
            out_ref[pl.ds(start, count), at(i, PAD), :] = (1.0 - DAMP) * v + moved

    loop(STRIPS[level], body)


def residual(level, v_ref, out_ref, b_ref, a_ref):
    def body(i):
        for start, count in solves(level, v_ref):
            v, moved = change(i, v_ref, b_ref, a_ref, start, count)
            out_ref[pl.ds(start, count), at(i, PAD), :] = a_ref[5, :, at(i, 0), :] * (moved - DAMP * v)

    loop(STRIPS[level], body)


def take(x, index):
    return jnp.take_along_axis(x, index, axis=1, mode="promise_in_bounds")


def quad_strip(ref, j, offset, tiles):
    base = pl.multiple_of(j * 16, 16) + offset
    lane = lax.broadcasted_iota(jnp.int32, (8, LANES), 1)
    even_lane = lax.rem(2 * lane, LANES)
    packed = []
    for t in tiles:
        pair = ref[t, pl.ds(base, 8, stride=2), :] + ref[t, pl.ds(base + 1, 8, stride=2), :]
        pair = pair + pltpu.roll(pair, LANES - 1, 1)
        packed.append(take(pair, even_lane))
    if len(packed) == 1:
        return [jnp.where(lane < LANES // 2, packed[0], 0.0)]
    return [jnp.where(lane < LANES // 2, packed[k], packed[k + 1]) for k in range(0, len(packed), 2)]


def restrict(count, ref, offset, tiles, store):
    def body(j):
        for k, q in enumerate(quad_strip(ref, j, offset, tiles)):
            store(j, k, q)

    loop(count, body)


def spread_strip(e_ref, j, offset, tiles):
    lane = lax.broadcasted_iota(jnp.int32, (8, LANES), 1)
    low = lax.div(lane, 2)
    high = low + LANES // 2
    rows = at(j, offset)
    out = []
    for t in tiles:
        e = e_ref[t, rows, :]
        out += [take(e, low), take(e, high)]
    return out


def prolong(count, e_ref, offset, e_tiles, v_ref, sign=1.0, v_offset=PAD, first=0):
    def body(j):
        base = pl.multiple_of(j * 16, 16) + v_offset
        for k, x in enumerate(spread_strip(e_ref, j, offset, e_tiles)):
            for parity in range(2):
                rows = pl.ds(base + parity, 8, stride=2)
                v_ref[first + k, rows, :] = v_ref[first + k, rows, :] + sign * x

    loop(count, body)


def clear_pads(*refs, value=0.0):
    for ref in refs:
        tiles, rows, _ = ref.shape
        ref[:, 0:PAD, :] = jnp.full((tiles, PAD, LANES), value, F32)
        ref[:, rows - PAD : rows, :] = jnp.full((tiles, PAD, LANES), value, F32)


def fill(ref, value):
    def body(i):
        ref[:, at(i, 0), :] = jnp.full((ref.shape[0], 8, LANES), value, F32)

    loop(ref.shape[1] // 8, body)


def pack_kernel(log_ref, src_ref, up_ref, down_ref):
    halo, own = HALO[0], OWN[0]
    up_ref[0:halo, :] = log_ref[own - halo : own, :]
    up_ref[halo : 2 * halo, :] = src_ref[own - halo : own, :]
    down_ref[0:halo, :] = log_ref[0:halo, :]
    down_ref[halo : 2 * halo, :] = src_ref[0:halo, :]


def first_row(level):
    return lax.axis_index("grid") * OWN[level] - HALO[level]


def scaled_store(bp_ref, a_ref, start=0, coarse_tiles=None):
    def store(j, k, q):
        tile = k if coarse_tiles is None else k % coarse_tiles
        bp_ref[start + k, at(j, PAD), :] = a_ref[4, tile, at(j, 0), :] * q

    return store


def quarter_store(c_ref):
    def store(j, k, q):
        c_ref[k, at(j, PAD), :] = 0.25 * q

    return store


def open_kernel(
    peers, log_ref, src_ref, above_ref, below_ref,
    msg_ref, a0_out, b0_out, v0_out, a1_out, b1_out, v1_out,
    c0, a0, bp0, va0, vb0, c1, a1, bp1, va1, vb1, sems,
):
    copies = []

    def send(src, dst):
        copy = pltpu.make_async_copy(src, dst, sems.at[len(copies)])
        copy.start()
        copies.append(copy)

    halo, own = HALO[0], OWN[0]
    clear_pads(c0, c1, value=1.0)
    clear_pads(bp0, va0, vb0, bp1, va1, vb1)

    def load(count, log_from, log_row, src_from, src_row, row):
        def body(i):
            logs = log_from[at(i, log_row), :]
            sources = src_from[at(i, src_row), :]
            for t in range(TILES[0]):
                c0[t, at(i, PAD + row), :] = jnp.exp(logs[:, t * LANES : (t + 1) * LANES])
                vb0[t, at(i, PAD + row), :] = sources[:, t * LANES : (t + 1) * LANES]

        loop(count // 8, body)

    load(halo, above_ref, 0, above_ref, halo, 0)
    load(own, log_ref, 0, src_ref, 0, halo)
    load(halo, below_ref, 0, below_ref, halo, halo + own)

    make_weights(0, c0, a0, first_row(0), peers * OWN[0])
    send(a0, a0_out)

    def scale(i):
        bp0[:, at(i, PAD), :] = a0[4, :, at(i, 0), :] * vb0[:, at(i, PAD), :]

    loop(STRIPS[0], scale)
    send(bp0, b0_out)
    restrict(STRIPS[1], c0, PAD, range(TILES[0]), quarter_store(c1))
    make_weights(1, c1, a1, first_row(1), peers * OWN[1])
    send(a1, a1_out)
    restrict(STRIPS[1], vb0, PAD, range(TILES[0]), scaled_store(bp1, a1, TILES[1], TILES[1]))
    relax(0, bp0, va0, bp0, a0)
    send(va0, v0_out)
    residual(0, va0, vb0, bp0, a0)
    restrict(STRIPS[1], vb0, PAD, range(TILES[0]), scaled_store(bp1, a1))
    send(bp1, b1_out)
    relax(1, bp1, va1, bp1, a1)
    send(va1, v1_out)
    residual(1, va1, vb1, bp1, a1)

    def store(j, k, q):
        msg_ref[k, at(j, 0), :] = q

    restrict(OWN[2] // 8, vb1, PAD + HALO[1], range(2 * TILES[1]), store)

    def store_coef(j, k, q):
        msg_ref[2 * TILES[2] + k, at(j, 0), :] = 0.25 * q

    restrict(OWN[2] // 8, c1, PAD + HALO[1], range(TILES[1]), store_coef)
    for copy in copies:
        copy.wait()


def deep_solve(a, bp, va, vb):
    relax(2, bp[2], va[2], bp[2], a[2])
    residual(2, va[2], vb[2], bp[2], a[2])
    for s in range(2):
        restrict(STRIPS[3], vb[2], PAD, range(s * 4, s * 4 + 4), scaled_store(bp[3], a[3], s * 2))
    relax(3, bp[3], va[3], bp[3], a[3])
    residual(3, va[3], vb[3], bp[3], a[3])
    for s in range(2):
        restrict(STRIPS[4], vb[3], PAD, range(s * 2, s * 2 + 2), scaled_store(bp[4], a[4], s))
    relax(4, bp[4], va[4], bp[4], a[4])
    relax(4, va[4], vb[4], bp[4], a[4])
    relax(4, vb[4], va[4], bp[4], a[4])
    prolong(STRIPS[4], va[4], PAD, range(2), va[3])
    relax(3, va[3], vb[3], bp[3], a[3])
    relax(3, vb[3], va[3], bp[3], a[3])
    prolong(STRIPS[3], va[3], PAD, range(4), va[2])
    relax(2, va[2], vb[2], bp[2], a[2])
    relax(2, vb[2], va[2], bp[2], a[2])


def up_level_1(va2, va1, vb1, bp1, a1):
    offset = PAD + HALO[2] - HALO[1] // 2
    prolong(4, va2, offset, range(2 * TILES[2]), va1)
    relax(1, va1, vb1, bp1, a1)
    relax(1, vb1, va1, bp1, a1)


def up_level_0(va1, va0, vb0, bp0, a0):
    prolong(STRIPS[1], va1, PAD, range(TILES[1]), va0)
    relax(0, va0, vb0, bp0, a0)
    relax(0, vb0, va0, bp0, a0)


def assemble(messages, a2, bp2):
    for slab, m in enumerate(messages):
        for i in range(2):
            row = slab * OWN[2] + i * 8
            for k in range(2 * TILES[2]):
                bp2[k, PAD + row : PAD + row + 8, :] = (
                    a2[4, k % TILES[2], row : row + 8, :] * m[k, i * 8 : i * 8 + 8, :]
                )


def middle_kernel(
    peers, m0, m1, m2, m3, m4, a0_in, b0_in, v0_in, a1_in, b1_in, v1_in,
    msg_ref, a2_out, a3_out, a4_out, v0_out, b1_out, v1_out,
    a0, bp0, va0, vb0, a1, bp1, va1, vb1,
    c2, a2, bp2, va2, vb2, c3, a3, bp3, va3, vb3, c4, a4, bp4, va4, vb4, sems,
):
    count = 0

    def start(src, dst):
        nonlocal count
        copy = pltpu.make_async_copy(src, dst, sems.at[count])
        copy.start()
        count += 1
        return copy

    loads = [start(s, d) for s, d in ((a1_in, a1), (b1_in, bp1), (v1_in, va1), (a0_in, a0), (b0_in, bp0), (v0_in, va0))]
    messages = (m0, m1, m2, m3, m4)
    fill(c4, 1.0)
    clear_pads(c2, c3, value=1.0)
    for ref in (bp4, va4, vb4):
        fill(ref, 0.0)
    clear_pads(bp2, va2, vb2, bp3, va3, vb3, vb0, vb1)
    top = first_row(2)
    for slab, m in enumerate(messages):
        for i in range(2):
            row = slab * OWN[2] + i * 8
            place = top + row + lax.broadcasted_iota(jnp.int32, (8, LANES), 0)
            inside = jnp.logical_and(place >= 0, place < peers * OWN[2])
            for k in range(TILES[2]):
                c2[k, PAD + row : PAD + row + 8, :] = jnp.where(
                    inside, m[2 * TILES[2] + k, i * 8 : i * 8 + 8, :], 1.0
                )
    make_weights(2, c2, a2, top, peers * OWN[2])
    restrict(STRIPS[3], c2, PAD, range(4), quarter_store(c3))
    make_weights(3, c3, a3, first_row(3), peers * OWN[3])
    restrict(2, c3, PAD, range(2), quarter_store(c4))

    def last_rows(j, k, q):
        keep = lax.broadcasted_iota(jnp.int32, (8, LANES), 0) < ROWS[4] - 16
        c4[k, PAD + 16 : PAD + 24, :] = jnp.where(keep, 0.25 * q, 1.0)

    restrict(1, c3, PAD + 32, range(2), last_rows)
    make_weights(4, c4, a4, first_row(4), peers * OWN[4])
    stores = [start(s, d) for s, d in ((a2, a2_out), (a3, a3_out), (a4, a4_out))]
    assemble(messages, a2, bp2)
    a = {2: a2, 3: a3, 4: a4}
    bp = {2: bp2, 3: bp3, 4: bp4}
    va = {2: va2, 3: va3, 4: va4}
    vb = {2: vb2, 3: vb3, 4: vb4}
    deep_solve(a, bp, va, vb)
    for copy in loads:
        copy.wait()
    up_level_1(va2, va1, vb1, bp1, a1)
    up_level_0(va1, va0, vb0, bp0, a0)

    relax(0, va0, vb0, bp0, a0)
    relax(0, vb0, va0, bp0, a0)
    stores.append(start(va0, v0_out))
    residual(0, va0, vb0, bp0, a0)
    restrict(STRIPS[1], vb0, PAD, range(TILES[0]), scaled_store(bp1, a1))
    stores.append(start(bp1, b1_out))

    def clear(i):
        va1[0 : TILES[1], at(i, 0), :] = jnp.zeros((TILES[1], 8, LANES), F32)

    loop(BUF[1] // 8, clear)
    relax(1, va1, vb1, bp1, a1)
    relax(1, vb1, va1, bp1, a1)
    stores.append(start(va1, v1_out))
    residual(1, va1, vb1, bp1, a1)

    def store(j, k, q):
        msg_ref[k, at(j, 0), :] = q

    restrict(OWN[2] // 8, vb1, PAD + HALO[1], range(2 * TILES[1]), store)
    for copy in stores:
        copy.wait()


def close_kernel(
    m0, m1, m2, m3, m4, a0_in, b0_in, v0_in, a1_in, b1_in, v1_in, a2_in, a3_in, a4_in,
    out_ref, mine_ref, other_ref,
    a0, bp0, va0, vb0, a1, bp1, va1, vb1,
    a2, bp2, va2, vb2, a3, bp3, va3, vb3, a4, bp4, va4, vb4, sems,
):
    count = 0

    def start(src, dst):
        nonlocal count
        copy = pltpu.make_async_copy(src, dst, sems.at[count])
        copy.start()
        count += 1
        return copy

    first = [start(s, d) for s, d in ((a2_in, a2), (a3_in, a3), (a4_in, a4))]
    loads = [start(s, d) for s, d in ((a1_in, a1), (b1_in, bp1), (v1_in, va1), (a0_in, a0), (b0_in, bp0), (v0_in, va0))]
    for ref in (bp4, va4, vb4):
        fill(ref, 0.0)
    clear_pads(bp2, va2, vb2, bp3, va3, vb3, vb0, vb1)
    for copy in first:
        copy.wait()
    assemble((m0, m1, m2, m3, m4), a2, bp2)
    a = {2: a2, 3: a3, 4: a4}
    bp = {2: bp2, 3: bp3, 4: bp4}
    va = {2: va2, 3: va3, 4: va4}
    vb = {2: vb2, 3: vb3, 4: vb4}
    deep_solve(a, bp, va, vb)
    for copy in loads:
        copy.wait()
    up_level_1(va2, va1, vb1, bp1, a1)
    up_level_0(va1, va0, vb0, bp0, a0)
    prolong(OWN[1] // 8, va1, PAD + HALO[1], range(TILES[1], 2 * TILES[1]), va0, -1.0, PAD + HALO[0])
    here = lax.axis_index("samp") * (TILES[0] // 2)
    there = TILES[0] // 2 - here

    def body(i):
        rows = at(i, PAD + HALO[0])
        for t in range(TILES[0]):
            out_ref[at(i, 0), t * LANES : (t + 1) * LANES] = va0[t, rows, :]
        for t in range(TILES[0] // 2):
            mine_ref[at(i, 0), t * LANES : (t + 1) * LANES] = va0[here + t, rows, :]
            other_ref[at(i, 0), t * LANES : (t + 1) * LANES] = va0[there + t, rows, :]

    loop(OWN[0] // 8, body)


VMEM = pl.BlockSpec(memory_space=pltpu.VMEM)
ANY = pl.BlockSpec(memory_space=pl.ANY)


def shape(*dims):
    return jax.ShapeDtypeStruct(dims, F32)


def a_shape(level):
    return (6, TILES[level], 8 * STRIPS[level], LANES)


def v_shape(level):
    return ((1 if level == 0 else 2) * TILES[level], BUF[level], LANES)


def c_shape(level):
    return (TILES[level], BUF[level], LANES)


def scratch(*shapes):
    return [pltpu.VMEM(s, F32) for s in shapes]


def level_scratch(level):
    return [a_shape(level)] + [v_shape(level)] * 3


def shifted(value, distance):
    peers = lax.axis_size("grid")
    pairs = [(i, i + distance) for i in range(peers) if 0 <= i + distance < peers]
    return lax.ppermute(value, "grid", pairs)


def gathered(value):
    return [shifted(value, 2), shifted(value, 1), value, shifted(value, -1), shifted(value, -2)]


def local(log_coef, source):
    peers = lax.axis_size("grid")
    log_field, source_field = log_coef[0], source[0]
    rows, columns = source_field.shape
    edge = shape(2 * HALO[0], columns)
    up, down = pl.pallas_call(
        pack_kernel, out_shape=(edge, edge), in_specs=[VMEM] * 2, out_specs=(VMEM, VMEM), name="pack"
    )(log_field, source_field)
    above, below = shifted(up, 1), shifted(down, -1)

    state = [a_shape(0), v_shape(0), v_shape(0), a_shape(1), v_shape(1), v_shape(1)]
    deep_state = [a_shape(2), a_shape(3), a_shape(4)]
    message, a0, b0, v0, a1, b1, v1 = pl.pallas_call(
        functools.partial(open_kernel, peers),
        out_shape=[shape(3 * TILES[2], OWN[2], LANES)] + [shape(*s) for s in state],
        in_specs=[VMEM] * 4,
        out_specs=[VMEM] + [ANY] * 6,
        scratch_shapes=scratch(c_shape(0), *level_scratch(0), c_shape(1), *level_scratch(1))
        + [pltpu.SemaphoreType.DMA((6,))],
        name="open",
    )(log_field, source_field, above, below)

    deep_scratch = [c_shape(2), *level_scratch(2), c_shape(3), *level_scratch(3), c_shape(4), *level_scratch(4)]
    message, a2, a3, a4, v0, b1, v1 = pl.pallas_call(
        functools.partial(middle_kernel, peers),
        out_shape=[shape(2 * TILES[2], OWN[2], LANES)] + [shape(*s) for s in deep_state + [state[1], state[4], state[5]]],
        in_specs=[VMEM] * 5 + [ANY] * 6,
        out_specs=[VMEM] + [ANY] * 6,
        scratch_shapes=scratch(*level_scratch(0), *level_scratch(1), *deep_scratch) + [pltpu.SemaphoreType.DMA((12,))],
        name="middle",
    )(*gathered(message), a0, b0, v0, a1, b1, v1)

    deep_scratch = [*level_scratch(2), *level_scratch(3), *level_scratch(4)]
    half = shape(rows, columns // 2)
    correction, mine, other = pl.pallas_call(
        close_kernel,
        out_shape=(shape(rows, columns), half, half),
        in_specs=[VMEM] * 5 + [ANY] * 9,
        out_specs=(VMEM,) * 3,
        scratch_shapes=scratch(*level_scratch(0), *level_scratch(1), *deep_scratch) + [pltpu.SemaphoreType.DMA((9,))],
        name="close",
    )(*gathered(message), a0, b0, v0, a1, b1, v1, a2, a3, a4)

    theirs = lax.ppermute(other, "samp", [(0, 1), (1, 0)])
    samples = lax.axis_size("samp")
    level_mean = (mine + theirs) / samples
    squares = mine * mine + theirs * theirs
    level_var = (squares - samples * level_mean * level_mean) / (samples - 1)
    return (correction[None], level_mean, level_var)


def solution(mesh):
    in_specs = (P("samp", "grid", None), P("samp", "grid", None))
    out_specs = (P("samp", "grid", None), P("grid", "samp"), P("grid", "samp"))
    return jax.shard_map(local, mesh=mesh, in_specs=in_specs, out_specs=out_specs, check_vma=False)
```

```python
import functools

import jax
import jax.numpy as jnp
from jax import lax
from jax.experimental import pallas as pl
from jax.experimental.pallas import tpu as pltpu
from jax.sharding import PartitionSpec as P

LANES = 128
PAD = 8
OWN = (64, 32, 16, 8, 4)
HALO = (24, 12, 32, 16, 8)
ROWS = tuple(o + 2 * h for o, h in zip(OWN, HALO))
TILES = (16, 8, 4, 2, 1)
STRIPS = (14, 7, 10, 5, 3)
BUF = tuple(8 * s + 2 * PAD for s in STRIPS)
SOLVES = (1, 2, 2, 2, 2)
UNROLL = (2, 7, 5, 5, 3)
DAMP = 0.8
F32 = jnp.float32


def loop(count, body, unroll=1):
    if unroll >= count:
        for i in range(count):
            body(i)
    else:
        lax.fori_loop(0, count, lambda i, c: (body(i), c)[1], 0, unroll=unroll)


def at(i, offset, step=8):
    if isinstance(i, int):
        return pl.ds(i * step + offset, 8)
    return pl.ds(pl.multiple_of(i * step, step) + offset, 8)


def pairs_at(i, offset):
    base = i * 16 if isinstance(i, int) else pl.multiple_of(i * 16, 16)
    return pl.ds(base + offset, 8, stride=2), pl.ds(base + offset + 1, 8, stride=2)


def iota(dim):
    return lax.broadcasted_iota(jnp.int32, (8, LANES), dim)


def side_values(x):
    return [pltpu.roll(x[-1], 1, 1)] + x[:-1], x[1:] + [pltpu.roll(x[0], LANES - 1, 1)]


def harmonic(a, b):
    return 2.0 * a * b / (a + b)


def make_weights(level, c_ref, a_ref, first_row, total_rows, source_ref=None, b_ref=None):
    tiles = TILES[level]

    def body(i):
        c = [c_ref[t, at(i, PAD), :] for t in range(tiles)]
        row = first_row + i * 8 + iota(0)
        lane = iota(1)
        inside = jnp.logical_and(row >= 0, row < total_rows)
        _, east = side_values(c)
        w_east = [harmonic(a, b) for a, b in zip(c, east)]
        w_west, _ = side_values(w_east)
        w_west[0] = jnp.where(lane == 0, harmonic(c[0], c[0]), w_west[0])
        w_east[-1] = jnp.where(lane == LANES - 1, harmonic(c[-1], c[-1]), w_east[-1])
        for t in range(tiles):
            w_north = harmonic(c[t], jnp.where(row == 0, c[t], c_ref[t, at(i, PAD - 1), :]))
            w_south = harmonic(c[t], jnp.where(row == total_rows - 1, c[t], c_ref[t, at(i, PAD + 1), :]))
            diagonal = w_west[t] + w_east[t] + w_north + w_south
            gain = jnp.where(inside, DAMP / diagonal, 0.0)
            a_west, a_east = gain * w_west[t], gain * w_east[t]
            if t == 0:
                a_west = jnp.where(lane == 0, 0.0, a_west)
            if t == tiles - 1:
                a_east = jnp.where(lane == LANES - 1, 0.0, a_east)
            rows = at(i, 0)
            a_ref[0, t, rows, :] = a_west
            a_ref[1, t, rows, :] = a_east
            a_ref[2, t, rows, :] = gain * w_north
            a_ref[3, t, rows, :] = gain * w_south
            a_ref[4, t, rows, :] = gain
            a_ref[5, t, rows, :] = diagonal * (1.0 / DAMP)
            if source_ref is not None:
                b_ref[t, at(i, PAD), :] = gain * source_ref[t, at(i, PAD), :]

    loop(STRIPS[level], body)


def sweep(level, v_ref, out_ref, b_ref, a_ref, finish):
    tiles, solves = TILES[level], SOLVES[level]

    def body(i):
        v = [[v_ref[s * tiles + t, at(i, PAD), :] for t in range(tiles)] for s in range(solves)]
        sides = [side_values(x) for x in v]
        rows = at(i, 0)
        order = list(range(1, tiles - 1)) + ([0, tiles - 1] if tiles > 1 else [0])
        for t in order:
            a_west, a_east, a_north, a_south = (a_ref[k, t, rows, :] for k in range(4))
            for s in range(solves):
                west, east = sides[s]
                k = s * tiles + t
                north, south = v_ref[k, at(i, PAD - 1), :], v_ref[k, at(i, PAD + 1), :]
                moved = (a_north * north + a_south * south) + b_ref[k, at(i, PAD), :]
                moved += a_west * west[t] + a_east * east[t]
                out_ref[k, at(i, PAD), :] = finish(v[s][t], moved, t, rows)

    loop(STRIPS[level], body, UNROLL[level])


def relax(level, v_ref, out_ref, b_ref, a_ref):
    sweep(level, v_ref, out_ref, b_ref, a_ref, lambda v, moved, t, rows: (1.0 - DAMP) * v + moved)


def residual(level, v_ref, out_ref, b_ref, a_ref):
    sweep(level, v_ref, out_ref, b_ref, a_ref, lambda v, moved, t, rows: a_ref[5, t, rows, :] * (moved - DAMP * v))


def restrict(count, ref, offset, tiles, store, unroll=1):
    def body(j):
        even, odd = pairs_at(j, offset)
        for k in range(0, len(tiles), 2):
            a, b = tiles[k], tiles[k + 1]
            store(j, k // 2, (ref[a, even, :] + ref[a, odd, :]) + (ref[b, even, :] + ref[b, odd, :]))

    loop(count, body, unroll)


def prolong(count, e_ref, offset, e_tiles, v_ref, sign=1.0, v_offset=PAD, unroll=1):
    def body(j):
        halves = pairs_at(j, v_offset)
        for k, tile in enumerate(e_tiles):
            e = sign * e_ref[tile, at(j, offset), :]
            for t in (2 * k, 2 * k + 1):
                for rows in halves:
                    v_ref[t, rows, :] = v_ref[t, rows, :] + e

    loop(count, body, unroll)


def clear_pads(*refs, value=0.0):
    for ref in refs:
        tiles, rows, _ = ref.shape
        ref[:, 0:PAD, :] = jnp.full((tiles, PAD, LANES), value, F32)
        ref[:, rows - PAD : rows, :] = jnp.full((tiles, PAD, LANES), value, F32)


def fill(ref, value):
    def body(i):
        ref[:, at(i, 0), :] = jnp.full((ref.shape[0], 8, LANES), value, F32)

    loop(ref.shape[1] // 8, body)


def take(x, index):
    return jnp.take_along_axis(x, index, axis=1, mode="promise_in_bounds")


def exchange_blocks(x):
    lane = iota(1)
    x = list(x)
    for step in (1, 2, 4, 8):
        upper = lax.rem(lane, 16 * step) >= 8 * step
        for i in range(16):
            if i & step == 0:
                j = i + step
                from_j = pltpu.roll(x[j], 8 * step, 1)
                from_i = pltpu.roll(x[i], LANES - 8 * step, 1)
                x[i], x[j] = jnp.where(upper, from_j, x[i]), jnp.where(upper, x[j], from_i)
    return x


def to_tiles(x):
    lane = iota(1)
    index = lax.rem(lane, 8) * 16 + lax.div(lane, 8)
    return exchange_blocks([take(v, index) for v in x])


def from_tiles(x):
    lane = iota(1)
    index = lax.rem(lane, 16) * 8 + lax.div(lane, 16)
    return [take(v, index) for v in exchange_blocks(x)]


def place():
    return lax.axis_index("grid")


def first_row(level):
    return place() * OWN[level] - HALO[level]


def towards_next():
    i = place()
    return lax.rem(i, 2) == 0, lax.rem(i, 4) < 2


def slab_positions():
    near, far = towards_next()
    return (
        jnp.where(near, 3, 1), jnp.where(near, 1, 3), jnp.where(far, 4, 0), jnp.where(far, 0, 4), 2,
    )


def pack_kernel(log_ref, src_ref, own_ref, first_ref, second_ref):
    halo, own = HALO[0], OWN[0]
    tiles = TILES[0]

    def body(i):
        rows = at(i, 0)
        for field, ref in enumerate((log_ref, src_ref)):
            x = [ref[rows, t * LANES : (t + 1) * LANES] for t in range(tiles)]
            if field == 0:
                x = [jnp.exp(v) for v in x]
            for t, v in enumerate(to_tiles(x)):
                own_ref[field * tiles + t, rows, :] = v

    loop(own // 8, body)
    near, _ = towards_next()
    start = jnp.where(near, own - halo, 0)
    for ref, base in ((first_ref, start), (second_ref, own - halo - start)):
        for i in range(halo // 8):
            from_rows = pl.ds(pl.multiple_of(base + 8 * i, 8), 8)
            for t in range(2 * tiles):
                ref[t, 8 * i : 8 * i + 8, :] = own_ref[t, from_rows, :]


def scaled_store(bp_ref, a_ref, start=0):
    def store(j, k, q):
        bp_ref[start + k, at(j, PAD), :] = a_ref[4, k, at(j, 0), :] * q

    return store


def quarter_store(c_ref):
    def store(j, k, q):
        c_ref[k, at(j, PAD), :] = 0.25 * q

    return store


class Copies:
    def __init__(self, sems):
        self.sems, self.count = sems, 0

    def start(self, *pairs):
        started = []
        for src, dst in pairs:
            copy = pltpu.make_async_copy(src, dst, self.sems.at[self.count])
            copy.start()
            self.count += 1
            started.append(copy)
        return started


def wait(copies):
    for copy in copies:
        copy.wait()


def open_kernel(
    peers, own_ref, first_ref, second_ref,
    msg_ref, a0_out, b0_out, v0_out, a1_out, b1_out, v1_out,
    c0, a0, bp0, va0, vb0, c1, a1, bp1, va1, vb1, sems,
):
    halo, own, tiles = HALO[0], OWN[0], TILES[0]
    copies = Copies(sems)
    near, _ = towards_next()
    first_at = pl.multiple_of(jnp.where(near, PAD + halo + own, PAD), 8)
    second_at = pl.multiple_of(jnp.where(near, PAD, PAD + halo + own), 8)
    loads = []
    for field, ref in enumerate((c0, vb0)):
        chunk = pl.ds(field * tiles, tiles)
        loads += copies.start(
            (own_ref.at[chunk], ref.at[:, PAD + halo : PAD + halo + own, :]),
            (first_ref.at[chunk], ref.at[:, pl.ds(first_at, halo), :]),
            (second_ref.at[chunk], ref.at[:, pl.ds(second_at, halo), :]),
        )
    clear_pads(c0, c1, value=1.0)
    clear_pads(bp0, va0, vb0, bp1, va1, vb1)
    wait(loads)
    make_weights(0, c0, a0, first_row(0), peers * OWN[0], vb0, bp0)
    stores = copies.start((a0, a0_out), (bp0, b0_out))
    restrict(STRIPS[1], c0, PAD, range(tiles), quarter_store(c1))
    make_weights(1, c1, a1, first_row(1), peers * OWN[1])
    stores += copies.start((a1, a1_out))
    restrict(STRIPS[1], vb0, PAD, range(tiles), scaled_store(bp1, a1, TILES[1]))
    relax(0, bp0, va0, bp0, a0)
    stores += copies.start((va0, v0_out))
    residual(0, va0, vb0, bp0, a0)
    restrict(STRIPS[1], vb0, PAD, range(tiles), scaled_store(bp1, a1))
    stores += copies.start((bp1, b1_out))
    relax(1, bp1, va1, bp1, a1)
    stores += copies.start((va1, v1_out))
    residual(1, va1, vb1, bp1, a1)

    def store(j, k, q):
        msg_ref[k, at(j, 0), :] = q

    restrict(OWN[2] // 8, vb1, PAD + HALO[1], range(2 * TILES[1]), store, 2)

    def store_coef(j, k, q):
        msg_ref[2 * TILES[2] + k, at(j, 0), :] = 0.25 * q

    restrict(OWN[2] // 8, c1, PAD + HALO[1], range(TILES[1]), store_coef, 2)
    wait(stores)


def deep_solve(a, bp, va, vb):
    relax(2, bp[2], va[2], bp[2], a[2])
    residual(2, va[2], vb[2], bp[2], a[2])
    for s in range(2):
        restrict(STRIPS[3], vb[2], PAD, range(s * 4, s * 4 + 4), scaled_store(bp[3], a[3], s * 2), 5)
    relax(3, bp[3], va[3], bp[3], a[3])
    residual(3, va[3], vb[3], bp[3], a[3])
    for s in range(2):
        restrict(STRIPS[4], vb[3], PAD, range(s * 2, s * 2 + 2), scaled_store(bp[4], a[4], s), 3)
    relax(4, bp[4], va[4], bp[4], a[4])
    relax(4, va[4], vb[4], bp[4], a[4])
    relax(4, vb[4], va[4], bp[4], a[4])
    prolong(STRIPS[4], va[4], PAD, range(2), va[3], unroll=3)
    relax(3, va[3], vb[3], bp[3], a[3])
    relax(3, vb[3], va[3], bp[3], a[3])
    prolong(STRIPS[3], va[3], PAD, range(4), va[2], unroll=5)
    relax(2, va[2], vb[2], bp[2], a[2])
    relax(2, vb[2], va[2], bp[2], a[2])


def up_level_1(va2, va1, vb1, bp1, a1):
    offset = PAD + HALO[2] - HALO[1] // 2
    prolong(4, va2, offset, range(2 * TILES[2]), va1)
    relax(1, va1, vb1, bp1, a1)
    relax(1, vb1, va1, bp1, a1)


def up_level_0(va1, va0, vb0, bp0, a0):
    prolong(STRIPS[1], va1, PAD, range(TILES[1]), va0)
    relax(0, va0, vb0, bp0, a0)
    relax(0, vb0, va0, bp0, a0)


def assemble(messages, a2, bp2):
    for position, m in zip(slab_positions(), messages):
        for i in range(2):
            row = pl.multiple_of(position * OWN[2] + i * 8, 8)
            for k in range(2 * TILES[2]):
                bp2[k, pl.ds(PAD + row, 8), :] = (
                    a2[4, k % TILES[2], pl.ds(row, 8), :] * m[k, i * 8 : i * 8 + 8, :]
                )


def middle_kernel(
    peers, m0, m1, m2, m3, m4, a0_in, b0_in, v0_in, a1_in, b1_in, v1_in,
    msg_ref, a2_out, a3_out, a4_out, v0_out, b1_out, v1_out,
    a0, bp0, va0, vb0, a1, bp1, va1, vb1,
    c2, a2, bp2, va2, vb2, c3, a3, bp3, va3, vb3, c4, a4, bp4, va4, vb4, sems,
):
    copies = Copies(sems)
    loads = copies.start((a1_in, a1), (b1_in, bp1), (v1_in, va1), (a0_in, a0), (b0_in, bp0), (v0_in, va0))
    messages = (m0, m1, m2, m3, m4)
    fill(c4, 1.0)
    clear_pads(c2, c3, value=1.0)
    for ref in (bp4, va4, vb4):
        fill(ref, 0.0)
    clear_pads(bp2, va2, vb2, bp3, va3, vb3, vb0, vb1)
    top = first_row(2)
    for position, m in zip(slab_positions(), messages):
        for i in range(2):
            row = pl.multiple_of(position * OWN[2] + i * 8, 8)
            for k in range(TILES[2]):
                c2[k, pl.ds(PAD + row, 8), :] = m[2 * TILES[2] + k, i * 8 : i * 8 + 8, :]
    make_weights(2, c2, a2, top, peers * OWN[2])
    restrict(STRIPS[3], c2, PAD, range(4), quarter_store(c3), 5)
    make_weights(3, c3, a3, first_row(3), peers * OWN[3])
    restrict(2, c3, PAD, range(2), quarter_store(c4), 2)

    def last_rows(j, k, q):
        c4[k, PAD + 16 : PAD + 24, :] = jnp.where(iota(0) < ROWS[4] - 16, 0.25 * q, 1.0)

    restrict(1, c3, PAD + 32, range(2), last_rows)
    make_weights(4, c4, a4, first_row(4), peers * OWN[4])
    stores = copies.start((a2, a2_out), (a3, a3_out), (a4, a4_out))
    assemble(messages, a2, bp2)
    a = {2: a2, 3: a3, 4: a4}
    bp = {2: bp2, 3: bp3, 4: bp4}
    va = {2: va2, 3: va3, 4: va4}
    vb = {2: vb2, 3: vb3, 4: vb4}
    deep_solve(a, bp, va, vb)
    wait(loads)
    up_level_1(va2, va1, vb1, bp1, a1)
    up_level_0(va1, va0, vb0, bp0, a0)

    relax(0, va0, vb0, bp0, a0)
    relax(0, vb0, va0, bp0, a0)
    stores += copies.start((va0, v0_out))
    residual(0, va0, vb0, bp0, a0)
    restrict(STRIPS[1], vb0, PAD, range(TILES[0]), scaled_store(bp1, a1))
    stores += copies.start((bp1, b1_out))

    def clear(i):
        va1[0 : TILES[1], at(i, 0), :] = jnp.zeros((TILES[1], 8, LANES), F32)

    loop(BUF[1] // 8, clear)
    relax(1, va1, vb1, bp1, a1)
    relax(1, vb1, va1, bp1, a1)
    stores += copies.start((va1, v1_out))
    residual(1, va1, vb1, bp1, a1)

    def store(j, k, q):
        msg_ref[k, at(j, 0), :] = q

    restrict(OWN[2] // 8, vb1, PAD + HALO[1], range(2 * TILES[1]), store, 2)
    wait(stores)


def close_kernel(
    m0, m1, m2, m3, m4, a0_in, b0_in, v0_in, a1_in, b1_in, v1_in, a2_in, a3_in, a4_in,
    out_ref, mine_ref, other_ref,
    a0, bp0, va0, vb0, a1, bp1, va1, vb1,
    a2, bp2, va2, vb2, a3, bp3, va3, vb3, a4, bp4, va4, vb4, sems,
):
    copies = Copies(sems)
    first = copies.start((a2_in, a2), (a3_in, a3), (a4_in, a4))
    loads = copies.start((a1_in, a1), (b1_in, bp1), (v1_in, va1), (a0_in, a0), (b0_in, bp0), (v0_in, va0))
    for ref in (bp4, va4, vb4):
        fill(ref, 0.0)
    clear_pads(bp2, va2, vb2, bp3, va3, vb3, vb0, vb1)
    wait(first)
    assemble((m0, m1, m2, m3, m4), a2, bp2)
    a = {2: a2, 3: a3, 4: a4}
    bp = {2: bp2, 3: bp3, 4: bp4}
    va = {2: va2, 3: va3, 4: va4}
    vb = {2: vb2, 3: vb3, 4: vb4}
    deep_solve(a, bp, va, vb)
    wait(loads)
    up_level_1(va2, va1, vb1, bp1, a1)
    up_level_0(va1, va0, vb0, bp0, a0)
    prolong(OWN[1] // 8, va1, PAD + HALO[1], range(TILES[1], 2 * TILES[1]), va0, -1.0, PAD + HALO[0])
    tiles = TILES[0]
    left = lax.axis_index("samp") == 0

    def body(i):
        x = from_tiles([va0[t, at(i, PAD + HALO[0]), :] for t in range(tiles)])
        for t in range(tiles):
            out_ref[at(i, 0), t * LANES : (t + 1) * LANES] = x[t]
        for t in range(tiles // 2):
            low, high = x[t], x[tiles // 2 + t]
            mine_ref[at(i, 0), t * LANES : (t + 1) * LANES] = jnp.where(left, low, high)
            other_ref[at(i, 0), t * LANES : (t + 1) * LANES] = jnp.where(left, high, low)

    loop(OWN[0] // 8, body)


VMEM = pl.BlockSpec(memory_space=pltpu.VMEM)
ANY = pl.BlockSpec(memory_space=pl.ANY)


def shape(*dims):
    return jax.ShapeDtypeStruct(dims, F32)


def a_shape(level):
    return (6, TILES[level], 8 * STRIPS[level], LANES)


def v_shape(level):
    return (SOLVES[level] * TILES[level], BUF[level], LANES)


def c_shape(level):
    return (TILES[level], BUF[level], LANES)


def scratch(*shapes):
    return [pltpu.VMEM(s, F32) for s in shapes]


def level_scratch(level):
    return [a_shape(level)] + [v_shape(level)] * 3


def swaps(distance):
    peers = lax.axis_size("grid")
    even = [(i, i + distance if i % (2 * distance) < distance else i - distance) for i in range(peers)]
    odd = [((a + distance) % peers, (b + distance) % peers) for a, b in even]
    return even, odd


def gathered(value):
    return [lax.ppermute(value, "grid", pairs) for distance in (1, 2) for pairs in swaps(distance)] + [value]


def local(log_coef, source):
    peers = lax.axis_size("grid")
    log_field, source_field = log_coef[0], source[0]
    rows, columns = source_field.shape
    edge = shape(2 * TILES[0], HALO[0], LANES)
    own, first, second = pl.pallas_call(
        pack_kernel,
        out_shape=(shape(2 * TILES[0], OWN[0], LANES), edge, edge),
        in_specs=[VMEM] * 2,
        out_specs=(VMEM,) * 3,
        name="pack",
    )(log_field, source_field)
    even, odd = swaps(1)
    first, second = lax.ppermute(first, "grid", even), lax.ppermute(second, "grid", odd)

    state = [a_shape(0), v_shape(0), v_shape(0), a_shape(1), v_shape(1), v_shape(1)]
    deep_state = [a_shape(2), a_shape(3), a_shape(4)]
    message, a0, b0, v0, a1, b1, v1 = pl.pallas_call(
        functools.partial(open_kernel, peers),
        out_shape=[shape(3 * TILES[2], OWN[2], LANES)] + [shape(*s) for s in state],
        in_specs=[ANY] * 3,
        out_specs=[VMEM] + [ANY] * 6,
        scratch_shapes=scratch(c_shape(0), *level_scratch(0), c_shape(1), *level_scratch(1))
        + [pltpu.SemaphoreType.DMA((12,))],
        name="open",
    )(own, first, second)

    deep_scratch = [c_shape(2), *level_scratch(2), c_shape(3), *level_scratch(3), c_shape(4), *level_scratch(4)]
    message, a2, a3, a4, v0, b1, v1 = pl.pallas_call(
        functools.partial(middle_kernel, peers),
        out_shape=[shape(2 * TILES[2], OWN[2], LANES)] + [shape(*s) for s in deep_state + [state[1], state[4], state[5]]],
        in_specs=[VMEM] * 5 + [ANY] * 6,
        out_specs=[VMEM] + [ANY] * 6,
        scratch_shapes=scratch(*level_scratch(0), *level_scratch(1), *deep_scratch) + [pltpu.SemaphoreType.DMA((12,))],
        name="middle",
    )(*gathered(message), a0, b0, v0, a1, b1, v1)

    deep_scratch = [*level_scratch(2), *level_scratch(3), *level_scratch(4)]
    half = shape(rows, columns // 2)
    correction, mine, other = pl.pallas_call(
        close_kernel,
        out_shape=(shape(rows, columns), half, half),
        in_specs=[VMEM] * 5 + [ANY] * 9,
        out_specs=(VMEM,) * 3,
        scratch_shapes=scratch(*level_scratch(0), *level_scratch(1), *deep_scratch) + [pltpu.SemaphoreType.DMA((9,))],
        name="close",
    )(*gathered(message), a0, b0, v0, a1, b1, v1, a2, a3, a4)

    theirs = lax.ppermute(other, "samp", [(0, 1), (1, 0)])
    samples = lax.axis_size("samp")
    level_mean = (mine + theirs) / samples
    squares = mine * mine + theirs * theirs
    level_var = (squares - samples * level_mean * level_mean) / (samples - 1)
    return (correction[None], level_mean, level_var)


def solution(mesh):
    in_specs = (P("samp", "grid", None), P("samp", "grid", None))
    out_specs = (P("samp", "grid", None), P("grid", "samp"), P("grid", "samp"))
    return jax.shard_map(local, mesh=mesh, in_specs=in_specs, out_specs=out_specs, check_vma=False)
```

```python
import functools

import jax
import jax.numpy as jnp
from jax import lax
from jax.experimental import pallas as pl
from jax.experimental.pallas import tpu as pltpu
from jax.sharding import PartitionSpec as P

LANES = 128
PAD = 8
OWN = (64, 32, 16, 8, 4)
HALO = (24, 12, 32, 16, 8)
ROWS = tuple(o + 2 * h for o, h in zip(OWN, HALO))
TILES = (16, 8, 4, 2, 1)
STRIPS = (14, 7, 10, 5, 3)
BUF = tuple(8 * s + 2 * PAD for s in STRIPS)
SOLVES = (1, 2, 2, 2, 2)
UNROLL = (2, 7, 5, 5, 3)
DAMP = 0.8
F32 = jnp.float32


def loop(count, body, unroll=1):
    first, last = count if isinstance(count, tuple) else (0, count)
    if unroll >= last - first:
        for i in range(first, last):
            body(i)
    else:
        lax.fori_loop(first, last, lambda i, c: (body(i), c)[1], 0, unroll=unroll)


def at(i, offset, step=8):
    if isinstance(i, int):
        return pl.ds(i * step + offset, 8)
    return pl.ds(pl.multiple_of(i * step, step) + offset, 8)


def pairs_at(i, offset):
    base = i * 16 if isinstance(i, int) else pl.multiple_of(i * 16, 16)
    return pl.ds(base + offset, 8, stride=2), pl.ds(base + offset + 1, 8, stride=2)


def iota(dim):
    return lax.broadcasted_iota(jnp.int32, (8, LANES), dim)


def from_west(x):
    return jnp.where(iota(1) < 16, pltpu.roll(x, 17, 1), pltpu.roll(x, 16, 1))


def from_east(x):
    return jnp.where(iota(1) >= LANES - 16, pltpu.roll(x, LANES - 17, 1), pltpu.roll(x, LANES - 16, 1))


def side_values(x):
    return [from_west(x[-1])] + x[:-1], x[1:] + [from_east(x[0])]


def harmonic(a, b):
    return 2.0 * a * b / (a + b)


def make_weights(level, c_ref, a_ref, first_row, total_rows, source_ref=None, b_ref=None):
    tiles = TILES[level]

    def body(i):
        c = [c_ref[t, at(i, PAD), :] for t in range(tiles)]
        row = first_row + i * 8 + iota(0)
        lane = iota(1)
        inside = jnp.logical_and(row >= 0, row < total_rows)
        _, east = side_values(c)
        w_east = [harmonic(a, b) for a, b in zip(c, east)]
        w_west, _ = side_values(w_east)
        w_west[0] = jnp.where(lane == 0, harmonic(c[0], c[0]), w_west[0])
        w_east[-1] = jnp.where(lane == LANES - 1, harmonic(c[-1], c[-1]), w_east[-1])
        for t in range(tiles):
            w_north = harmonic(c[t], jnp.where(row == 0, c[t], c_ref[t, at(i, PAD - 1), :]))
            w_south = harmonic(c[t], jnp.where(row == total_rows - 1, c[t], c_ref[t, at(i, PAD + 1), :]))
            diagonal = w_west[t] + w_east[t] + w_north + w_south
            gain = jnp.where(inside, DAMP / diagonal, 0.0)
            a_west, a_east = gain * w_west[t], gain * w_east[t]
            if t == 0:
                a_west = jnp.where(lane == 0, 0.0, a_west)
            if t == tiles - 1:
                a_east = jnp.where(lane == LANES - 1, 0.0, a_east)
            rows = at(i, 0)
            a_ref[0, t, rows, :] = a_west
            a_ref[1, t, rows, :] = a_east
            a_ref[2, t, rows, :] = gain * w_north
            a_ref[3, t, rows, :] = gain * w_south
            a_ref[4, t, rows, :] = gain
            a_ref[5, t, rows, :] = diagonal * (1.0 / DAMP)
            if source_ref is not None:
                b_ref[t, at(i, PAD), :] = gain * source_ref[t, at(i, PAD), :]

    loop(STRIPS[level], body)


def sweep(level, v_ref, out_ref, b_ref, a_ref, finish, strips):
    tiles, solves = TILES[level], SOLVES[level]

    def body(i):
        v = [[v_ref[s * tiles + t, at(i, PAD), :] for t in range(tiles)] for s in range(solves)]
        sides = [side_values(x) for x in v]
        rows = at(i, 0)
        order = list(range(1, tiles - 1)) + ([0, tiles - 1] if tiles > 1 else [0])
        for t in order:
            a_west, a_east, a_north, a_south = (a_ref[k, t, rows, :] for k in range(4))
            for s in range(solves):
                west, east = sides[s]
                k = s * tiles + t
                north, south = v_ref[k, at(i, PAD - 1), :], v_ref[k, at(i, PAD + 1), :]
                moved = (a_north * north + a_south * south) + b_ref[k, at(i, PAD), :]
                moved += a_west * west[t] + a_east * east[t]
                out_ref[k, at(i, PAD), :] = finish(v[s][t], moved, t, rows)

    loop(strips or STRIPS[level], body, UNROLL[level])


def relax(level, v_ref, out_ref, b_ref, a_ref, strips=None):
    sweep(level, v_ref, out_ref, b_ref, a_ref, lambda v, moved, t, rows: (1.0 - DAMP) * v + moved, strips)


def residual(level, v_ref, out_ref, b_ref, a_ref, strips=None):
    def finish(v, moved, t, rows):
        return a_ref[5, t, rows, :] * (moved - DAMP * v)

    sweep(level, v_ref, out_ref, b_ref, a_ref, finish, strips)


def restrict(count, ref, offset, tiles, store, unroll=1):
    def body(j):
        even, odd = pairs_at(j, offset)
        for k in range(0, len(tiles), 2):
            a, b = tiles[k], tiles[k + 1]
            store(j, k // 2, (ref[a, even, :] + ref[a, odd, :]) + (ref[b, even, :] + ref[b, odd, :]))

    loop(count, body, unroll)


def prolong(count, e_ref, offset, e_tiles, v_ref, sign=1.0, v_offset=PAD, unroll=1):
    def body(j):
        halves = pairs_at(j, v_offset)
        for k, tile in enumerate(e_tiles):
            e = sign * e_ref[tile, at(j, offset), :]
            for t in (2 * k, 2 * k + 1):
                for rows in halves:
                    v_ref[t, rows, :] = v_ref[t, rows, :] + e

    loop(count, body, unroll)


def clear_pads(*refs, value=0.0, size=PAD):
    for ref in refs:
        tiles, rows, _ = ref.shape
        ref[:, 0:size, :] = jnp.full((tiles, size, LANES), value, F32)
        ref[:, rows - size : rows, :] = jnp.full((tiles, size, LANES), value, F32)


def fill(ref, value):
    def body(i):
        ref[:, at(i, 0), :] = jnp.full((ref.shape[0], 8, LANES), value, F32)

    loop(ref.shape[1] // 8, body)


def turn(groups):
    lane = iota(1)
    groups = [list(x) for x in groups]
    for step in (1, 2, 4, 8):
        upper = lax.rem(lane, 2 * step) >= step
        for i in range(16):
            if i & step == 0:
                j = i + step
                for x in groups:
                    from_j = pltpu.roll(x[j], step, 1)
                    from_i = pltpu.roll(x[i], LANES - step, 1)
                    x[i], x[j] = jnp.where(upper, from_j, x[i]), jnp.where(upper, x[j], from_i)
    return groups


def place():
    return lax.axis_index("grid")


def first_row(level):
    return place() * OWN[level] - HALO[level]


def towards_next():
    i = place()
    return lax.rem(i, 2) == 0, lax.rem(i, 4) < 2


def slab_positions():
    next_first, far = towards_next()
    return (
        jnp.where(next_first, 3, 1), jnp.where(next_first, 1, 3), jnp.where(far, 4, 0), jnp.where(far, 0, 4), 2,
    )


def pack_kernel(log_ref, src_ref, c0, s0, first_ref, second_ref):
    halo, own = HALO[0], OWN[0]
    tiles = TILES[0]

    def body(i):
        logs, sources = ([ref[at(i, 0), t * LANES : (t + 1) * LANES] for t in range(tiles)] for ref in (log_ref, src_ref))
        for ref, x in zip((c0, s0), turn(([jnp.exp(v) for v in logs], sources))):
            for t, v in enumerate(x):
                ref[t, at(i, PAD + halo), :] = v

    loop(own // 8, body)
    next_first, _ = towards_next()
    start = jnp.where(next_first, own - halo, 0)
    for ref, base in ((first_ref, start), (second_ref, own - halo - start)):
        for i in range(halo // 8):
            rows = pl.ds(pl.multiple_of(PAD + halo + base + 8 * i, 8), 8)
            for t in range(tiles):
                ref[t, 8 * i : 8 * i + 8, :] = c0[t, rows, :]
                ref[tiles + t, 8 * i : 8 * i + 8, :] = s0[t, rows, :]


def scaled_store(bp_ref, a_ref, start=0):
    def store(j, k, q):
        bp_ref[start + k, at(j, PAD), :] = a_ref[4, k, at(j, 0), :] * q

    return store


def quarter_store(c_ref):
    def store(j, k, q):
        c_ref[k, at(j, PAD), :] = 0.25 * q

    return store


def open_kernel(
    peers, c0_in, s0_in, first_ref, second_ref,
    c0, s0, msg_ref, a0, bp0, va0, a1, bp1, va1,
    vb0, c1, vb1,
):
    halo, own, tiles = HALO[0], OWN[0], TILES[0]
    next_first, _ = towards_next()
    above, below = PAD, PAD + halo + own
    for ref, base in ((first_ref, jnp.where(next_first, below, above)), (second_ref, jnp.where(next_first, above, below))):
        for i in range(halo // 8):
            rows = pl.ds(pl.multiple_of(base + 8 * i, 8), 8)
            for t in range(tiles):
                c0[t, rows, :] = ref[t, 8 * i : 8 * i + 8, :]
                s0[t, rows, :] = ref[tiles + t, 8 * i : 8 * i + 8, :]
    clear_pads(c0, c1, value=1.0)
    clear_pads(bp0, va0, vb0, bp1, va1, vb1)
    make_weights(0, c0, a0, first_row(0), peers * OWN[0], s0, bp0)
    restrict(STRIPS[1], c0, PAD, range(tiles), quarter_store(c1))
    make_weights(1, c1, a1, first_row(1), peers * OWN[1])
    restrict(STRIPS[1], s0, PAD, range(tiles), scaled_store(bp1, a1, TILES[1]))
    relax(0, bp0, va0, bp0, a0)
    residual(0, va0, vb0, bp0, a0)
    restrict(STRIPS[1], vb0, PAD, range(tiles), scaled_store(bp1, a1))
    relax(1, bp1, va1, bp1, a1)
    residual(1, va1, vb1, bp1, a1, (1, 6))

    def store(j, k, q):
        msg_ref[k, at(j, 0), :] = q

    restrict(OWN[2] // 8, vb1, PAD + HALO[1], range(2 * TILES[1]), store, 2)

    def store_coef(j, k, q):
        msg_ref[2 * TILES[2] + k, at(j, 0), :] = 0.25 * q

    restrict(OWN[2] // 8, c1, PAD + HALO[1], range(TILES[1]), store_coef, 2)


def deep_solve(a, bp, va, vb):
    relax(2, bp[2], va[2], bp[2], a[2])
    residual(2, va[2], vb[2], bp[2], a[2])
    for s in range(2):
        restrict(STRIPS[3], vb[2], PAD, range(s * 4, s * 4 + 4), scaled_store(bp[3], a[3], s * 2), 5)
    relax(3, bp[3], va[3], bp[3], a[3])
    residual(3, va[3], vb[3], bp[3], a[3])
    for s in range(2):
        restrict(STRIPS[4], vb[3], PAD, range(s * 2, s * 2 + 2), scaled_store(bp[4], a[4], s), 3)
    relax(4, bp[4], va[4], bp[4], a[4])
    relax(4, va[4], vb[4], bp[4], a[4])
    relax(4, vb[4], va[4], bp[4], a[4])
    prolong(2, va[4], PAD, range(2), va[3], unroll=2)
    relax(3, va[3], vb[3], bp[3], a[3], (0, 5))
    relax(3, vb[3], va[3], bp[3], a[3], (1, 4))
    prolong((1, 4), va[3], PAD, range(4), va[2], unroll=3)
    relax(2, va[2], vb[2], bp[2], a[2], (3, 7))
    relax(2, vb[2], va[2], bp[2], a[2], (3, 7))


def up_level_1(va2, va1, vb1, bp1, a1, strips=(0, 7)):
    offset = PAD + HALO[2] - HALO[1] // 2
    prolong(4, va2, offset, range(2 * TILES[2]), va1)
    relax(1, va1, vb1, bp1, a1, strips)
    relax(1, vb1, va1, bp1, a1, strips)


def up_level_0(va1, va0, vb0, bp0, a0, first, second):
    prolong(STRIPS[1], va1, PAD, range(TILES[1]), va0)
    relax(0, va0, vb0, bp0, a0, first)
    relax(0, vb0, va0, bp0, a0, second)


def assemble(messages, a2, bp2):
    for position, m in zip(slab_positions(), messages):
        for i in range(2):
            row = pl.multiple_of(position * OWN[2] + i * 8, 8)
            for k in range(2 * TILES[2]):
                bp2[k, pl.ds(PAD + row, 8), :] = (
                    a2[4, k % TILES[2], pl.ds(row, 8), :] * m[k, i * 8 : i * 8 + 8, :]
                )


def middle_kernel(
    peers, m0, m1, m2, m3, m4, a0, bp0, va0_in, a1, bp1_in, va1_in,
    msg_ref, a2, a3, a4, va0, bp1, va1,
    vb0, vb1, c2, bp2, va2, vb2, c3, bp3, va3, vb3, c4, bp4, va4, vb4,
):
    messages = (m0, m1, m2, m3, m4)
    fill(c4, 1.0)
    clear_pads(c2, c3, value=1.0)
    for ref in (bp4, va4, vb4):
        fill(ref, 0.0)
    clear_pads(bp2, va2, vb2, bp3, va3, vb3)
    clear_pads(vb0, vb1, size=2 * PAD)
    top = first_row(2)
    for position, m in zip(slab_positions(), messages):
        for i in range(2):
            row = pl.multiple_of(position * OWN[2] + i * 8, 8)
            for k in range(TILES[2]):
                c2[k, pl.ds(PAD + row, 8), :] = m[2 * TILES[2] + k, i * 8 : i * 8 + 8, :]
    make_weights(2, c2, a2, top, peers * OWN[2])
    restrict(STRIPS[3], c2, PAD, range(4), quarter_store(c3), 5)
    make_weights(3, c3, a3, first_row(3), peers * OWN[3])
    restrict(2, c3, PAD, range(2), quarter_store(c4), 2)

    def last_rows(j, k, q):
        c4[k, PAD + 16 : PAD + 24, :] = jnp.where(iota(0) < ROWS[4] - 16, 0.25 * q, 1.0)

    restrict(1, c3, PAD + 32, range(2), last_rows)
    make_weights(4, c4, a4, first_row(4), peers * OWN[4])
    assemble(messages, a2, bp2)
    a = {2: a2, 3: a3, 4: a4}
    bp = {2: bp2, 3: bp3, 4: bp4}
    va = {2: va2, 3: va3, 4: va4}
    vb = {2: vb2, 3: vb3, 4: vb4}
    deep_solve(a, bp, va, vb)
    up_level_1(va2, va1, vb1, bp1, a1)
    up_level_0(va1, va0, vb0, bp0, a0, (1, 13), (1, 13))

    relax(0, va0, vb0, bp0, a0, (1, 13))
    relax(0, vb0, va0, bp0, a0, (1, 13))
    residual(0, va0, vb0, bp0, a0, (1, 13))
    restrict((1, 6), vb0, PAD, range(TILES[0]), scaled_store(bp1, a1))

    def clear(i):
        va1[0 : TILES[1], at(i, 0), :] = jnp.zeros((TILES[1], 8, LANES), F32)

    loop(BUF[1] // 8, clear)
    relax(1, va1, vb1, bp1, a1)
    relax(1, vb1, va1, bp1, a1)
    residual(1, va1, vb1, bp1, a1, (1, 6))

    def store(j, k, q):
        msg_ref[k, at(j, 0), :] = q

    restrict(OWN[2] // 8, vb1, PAD + HALO[1], range(2 * TILES[1]), store, 2)


def close_kernel(
    m0, m1, m2, m3, m4, a0, bp0, va0_in, a1, bp1, va1_in, a2, a3, a4,
    va0, va1, out_ref, mine_ref, other_ref,
    vb0, vb1, bp2, va2, vb2, bp3, va3, vb3, bp4, va4, vb4,
):
    for ref in (bp4, va4, vb4):
        fill(ref, 0.0)
    clear_pads(bp2, va2, vb2, bp3, va3, vb3)
    clear_pads(vb0, vb1, size=2 * PAD)
    assemble((m0, m1, m2, m3, m4), a2, bp2)
    a = {2: a2, 3: a3, 4: a4}
    bp = {2: bp2, 3: bp3, 4: bp4}
    va = {2: va2, 3: va3, 4: va4}
    vb = {2: vb2, 3: vb3, 4: vb4}
    deep_solve(a, bp, va, vb)
    up_level_1(va2, va1, vb1, bp1, a1, (1, 6))
    up_level_0(va1, va0, vb0, bp0, a0, (2, 12), (3, 11))
    prolong(OWN[1] // 8, va1, PAD + HALO[1], range(TILES[1], 2 * TILES[1]), va0, -1.0, PAD + HALO[0])
    tiles = TILES[0]
    left = lax.axis_index("samp") == 0

    def body(i):
        strips = (2 * i, 2 * i + 1)
        turned = turn([[va0[t, at(j, PAD + HALO[0]), :] for t in range(tiles)] for j in strips])
        for j, x in zip(strips, turned):
            for t in range(tiles):
                out_ref[at(j, 0), t * LANES : (t + 1) * LANES] = x[t]
            for t in range(tiles // 2):
                low, high = x[t], x[tiles // 2 + t]
                mine_ref[at(j, 0), t * LANES : (t + 1) * LANES] = jnp.where(left, low, high)
                other_ref[at(j, 0), t * LANES : (t + 1) * LANES] = jnp.where(left, high, low)

    loop(OWN[0] // 16, body)


VMEM = pl.BlockSpec(memory_space=pltpu.VMEM)


def near(*dims):
    return pltpu.VMEM(dims, F32)


def held(*values):
    return [pltpu.with_memory_space_constraint(v, pltpu.VMEM) for v in values]


def a_shape(level):
    return (6, TILES[level], 8 * STRIPS[level], LANES)


def v_shape(level):
    return (SOLVES[level] * TILES[level], BUF[level], LANES)


def c_shape(level):
    return (TILES[level], BUF[level], LANES)


def call(kernel, name, arguments, outputs, scratch=(), aliases=None):
    return pl.pallas_call(
        kernel,
        out_shape=outputs,
        in_specs=[VMEM] * len(arguments),
        out_specs=[VMEM] * len(outputs),
        scratch_shapes=[pltpu.VMEM(s, F32) for s in scratch],
        input_output_aliases=aliases or {},
        compiler_params=pltpu.CompilerParams(vmem_limit_bytes=24 * 2**20),
        name=name,
    )(*arguments)


def swaps(distance):
    peers = lax.axis_size("grid")
    even = [(i, i + distance if i % (2 * distance) < distance else i - distance) for i in range(peers)]
    odd = [((a + distance) % peers, (b + distance) % peers) for a, b in even]
    return even, odd


def gathered(value):
    return [lax.ppermute(value, "grid", pairs) for distance in (1, 2) for pairs in swaps(distance)] + [value]


def local(log_coef, source):
    peers = lax.axis_size("grid")
    log_field, source_field = log_coef[0], source[0]
    rows, columns = source_field.shape
    edge = near(2 * TILES[0], HALO[0], LANES)
    c0, s0, first, second = call(
        pack_kernel, "pack", (log_field, source_field), (near(*c_shape(0)), near(*c_shape(0)), edge, edge)
    )
    even, odd = swaps(1)
    first, second = lax.ppermute(first, "grid", even), lax.ppermute(second, "grid", odd)

    state = [near(*f(level)) for level in (0, 1) for f in (a_shape, v_shape, v_shape)]
    c0, s0, message, a0, b0, v0, a1, b1, v1 = call(
        functools.partial(open_kernel, peers),
        "open",
        held(c0, s0, first, second),
        [near(*c_shape(0)), near(*c_shape(0)), near(3 * TILES[2], OWN[2], LANES)] + state,
        [v_shape(0), c_shape(1), v_shape(1)],
        {0: 0, 1: 1},
    )
    deep = [shape for level in (2, 3, 4) for shape in [c_shape(level)] + [v_shape(level)] * 3]
    message, a2, a3, a4, v0, b1, v1 = call(
        functools.partial(middle_kernel, peers),
        "middle",
        held(*gathered(message), a0, b0, v0, a1, b1, v1),
        [near(2 * TILES[2], OWN[2], LANES)] + [near(*a_shape(level)) for level in (2, 3, 4)] + [state[k] for k in (2, 4, 5)],
        [v_shape(0), v_shape(1)] + deep,
        {7: 4, 9: 5, 10: 6},
    )
    deep = [shape for level in (2, 3, 4) for shape in [v_shape(level)] * 3]
    half = near(rows, columns // 2)
    v0, v1, correction, mine, other = call(
        close_kernel,
        "close",
        held(*gathered(message), a0, b0, v0, a1, b1, v1, a2, a3, a4),
        (state[2], state[5], jax.ShapeDtypeStruct((rows, columns), F32), half, half),
        [v_shape(0), v_shape(1)] + deep,
        {7: 0, 10: 1},
    )

    theirs = lax.ppermute(other, "samp", [(0, 1), (1, 0)])
    samples = lax.axis_size("samp")
    level_mean = (mine + theirs) / samples
    squares = mine * mine + theirs * theirs
    level_var = (squares - samples * level_mean * level_mean) / (samples - 1)
    return (correction[None], level_mean, level_var)


def solution(mesh):
    in_specs = (P("samp", "grid", None), P("samp", "grid", None))
    out_specs = (P("samp", "grid", None), P("grid", "samp"), P("grid", "samp"))
    return jax.shard_map(local, mesh=mesh, in_specs=in_specs, out_specs=out_specs, check_vma=False)
```

```python
import functools

import jax
import jax.numpy as jnp
from jax import lax
from jax.experimental import pallas as pl
from jax.experimental.pallas import tpu as pltpu
from jax.sharding import PartitionSpec as P

LANES = 128
PAD = 8
OWN = (64, 32, 16, 8, 4)
HALO = (24, 12, 32, 16, 8)
ROWS = tuple(o + 2 * h for o, h in zip(OWN, HALO))
TILES = (16, 8, 4, 2, 1)
STRIPS = (14, 7, 10, 5, 3)
BUF = tuple(8 * s + 2 * PAD for s in STRIPS)
SOLVES = (1, 2, 2, 2, 2)
UNROLL = (2, 7, 5, 5, 3)
DAMP = 0.8
F32 = jnp.float32


def loop(count, body, unroll=1):
    first, last = count if isinstance(count, tuple) else (0, count)
    if unroll >= last - first:
        for i in range(first, last):
            body(i)
    else:
        lax.fori_loop(first, last, lambda i, c: (body(i), c)[1], 0, unroll=unroll)


def at(i, offset, step=8):
    if isinstance(i, int):
        return pl.ds(i * step + offset, 8)
    return pl.ds(pl.multiple_of(i * step, step) + offset, 8)


def pairs_at(i, offset):
    base = i * 16 if isinstance(i, int) else pl.multiple_of(i * 16, 16)
    return pl.ds(base + offset, 8, stride=2), pl.ds(base + offset + 1, 8, stride=2)


def iota(dim):
    return lax.broadcasted_iota(jnp.int32, (8, LANES), dim)


def from_west(x):
    return jnp.where(iota(1) < 16, pltpu.roll(x, 17, 1), pltpu.roll(x, 16, 1))


def from_east(x):
    return jnp.where(iota(1) >= LANES - 16, pltpu.roll(x, LANES - 17, 1), pltpu.roll(x, LANES - 16, 1))


def side_values(x):
    return [from_west(x[-1])] + x[:-1], x[1:] + [from_east(x[0])]


def harmonic(a, b):
    return 2.0 * a * b / (a + b)


def make_weights(level, c_ref, a_ref, peers, strips=None, source_ref=None, b_ref=None):
    tiles = TILES[level]
    top, total_rows = first_row(level), peers * OWN[level]

    def body(i):
        c = [c_ref[t, at(i, PAD), :] for t in range(tiles)]
        row = top + i * 8 + iota(0)
        lane = iota(1)
        inside = jnp.logical_and(row >= 0, row < total_rows)
        west, east = side_values(c)
        west[0] = jnp.where(lane == 0, c[0], west[0])
        east[-1] = jnp.where(lane == LANES - 1, c[-1], east[-1])
        w_east = [harmonic(a, b) for a, b in zip(c, east)]
        w_west = [harmonic(c[0], west[0])] + w_east[:-1]
        for t in range(tiles):
            w_north = harmonic(c[t], jnp.where(row == 0, c[t], c_ref[t, at(i, PAD - 1), :]))
            w_south = harmonic(c[t], jnp.where(row == total_rows - 1, c[t], c_ref[t, at(i, PAD + 1), :]))
            diagonal = w_west[t] + w_east[t] + w_north + w_south
            gain = jnp.where(inside, DAMP / diagonal, 0.0)
            a_west, a_east = gain * w_west[t], gain * w_east[t]
            if t == 0:
                a_west = jnp.where(lane == 0, 0.0, a_west)
            if t == tiles - 1:
                a_east = jnp.where(lane == LANES - 1, 0.0, a_east)
            rows = at(i, 0)
            a_ref[0, t, rows, :] = a_west
            a_ref[1, t, rows, :] = a_east
            a_ref[2, t, rows, :] = gain * w_north
            a_ref[3, t, rows, :] = gain * w_south
            a_ref[4, t, rows, :] = gain
            a_ref[5, t, rows, :] = diagonal * (1.0 / DAMP)
            if source_ref is not None:
                b_ref[t, at(i, PAD), :] = gain * source_ref[t, at(i, PAD), :]

    loop(strips or STRIPS[level], body, UNROLL[level])


def sweep(level, v_ref, out_ref, b_ref, a_ref, finish, strips):
    tiles, solves = TILES[level], SOLVES[level]

    def body(i):
        v = [[v_ref[s * tiles + t, at(i, PAD), :] for t in range(tiles)] for s in range(solves)]
        sides = [side_values(x) for x in v]
        rows = at(i, 0)
        order = list(range(1, tiles - 1)) + ([0, tiles - 1] if tiles > 1 else [0])
        for t in order:
            a_west, a_east, a_north, a_south = (a_ref[k, t, rows, :] for k in range(4))
            for s in range(solves):
                west, east = sides[s]
                k = s * tiles + t
                north, south = v_ref[k, at(i, PAD - 1), :], v_ref[k, at(i, PAD + 1), :]
                moved = (a_north * north + a_south * south) + b_ref[k, at(i, PAD), :]
                moved += a_west * west[t] + a_east * east[t]
                out_ref[k, at(i, PAD), :] = finish(v[s][t], moved, t, rows)

    loop(strips or STRIPS[level], body, UNROLL[level])


def relax(level, v_ref, out_ref, b_ref, a_ref, strips=None):
    sweep(level, v_ref, out_ref, b_ref, a_ref, lambda v, moved, t, rows: (1.0 - DAMP) * v + moved, strips)


def residual(level, v_ref, out_ref, b_ref, a_ref, strips=None):
    def finish(v, moved, t, rows):
        return a_ref[5, t, rows, :] * (moved - DAMP * v)

    sweep(level, v_ref, out_ref, b_ref, a_ref, finish, strips)


def restrict(count, ref, offset, tiles, store, unroll=1):
    def body(j):
        even, odd = pairs_at(j, offset)
        for k in range(0, len(tiles), 2):
            a, b = tiles[k], tiles[k + 1]
            store(j, k // 2, (ref[a, even, :] + ref[a, odd, :]) + (ref[b, even, :] + ref[b, odd, :]))

    loop(count, body, unroll)


def prolong(count, e_ref, offset, e_tiles, v_ref, sign=1.0, v_offset=PAD, unroll=1):
    def body(j):
        halves = pairs_at(j, v_offset)
        for k, tile in enumerate(e_tiles):
            e = sign * e_ref[tile, at(j, offset), :]
            for t in (2 * k, 2 * k + 1):
                for rows in halves:
                    v_ref[t, rows, :] = v_ref[t, rows, :] + e

    loop(count, body, unroll)


def clear_pads(*refs, value=0.0, size=PAD):
    for ref in refs:
        tiles, rows, _ = ref.shape
        ref[:, 0:size, :] = jnp.full((tiles, size, LANES), value, F32)
        ref[:, rows - size : rows, :] = jnp.full((tiles, size, LANES), value, F32)


def fill(ref, value):
    def body(i):
        ref[:, at(i, 0), :] = jnp.full((ref.shape[0], 8, LANES), value, F32)

    loop(ref.shape[1] // 8, body)


def turn(groups):
    lane = iota(1)
    groups = [list(x) for x in groups]
    for step in (1, 2, 4, 8):
        upper = lax.rem(lane, 2 * step) >= step
        for i in range(16):
            if i & step == 0:
                j = i + step
                for x in groups:
                    from_j = pltpu.roll(x[j], step, 1)
                    from_i = pltpu.roll(x[i], LANES - step, 1)
                    x[i], x[j] = jnp.where(upper, from_j, x[i]), jnp.where(upper, x[j], from_i)
    return groups


def place():
    return lax.axis_index("grid")


def first_row(level):
    return place() * OWN[level] - HALO[level]


def towards_next():
    i = place()
    return lax.rem(i, 2) == 0, lax.rem(i, 4) < 2


def slab_positions():
    next_first, far = towards_next()
    return (
        jnp.where(next_first, 3, 1), jnp.where(next_first, 1, 3), jnp.where(far, 4, 0), jnp.where(far, 0, 4), 2,
    )


def convert(rows_of, log_ref, src_ref, c0, s0):
    tiles = TILES[0]
    for row, to in rows_of:
        logs, sources = ([ref[row : row + 8, t * LANES : (t + 1) * LANES] for t in range(tiles)] for ref in (log_ref, src_ref))
        for ref, x in zip((c0, s0), turn(([jnp.exp(v) for v in logs], sources))):
            for t, v in enumerate(x):
                ref[t, to : to + 8, :] = v


def load(sems, *pairs):
    copies = [pltpu.make_async_copy(src, dst, sems.at[k]) for k, (src, dst) in enumerate(pairs)]
    for copy in copies:
        copy.start()
    return copies


def pack_kernel(log_in, src_in, c0, s0, first_ref, second_ref, logs, sources, sems):
    halo, own, tiles = HALO[0], OWN[0], TILES[0]
    pairs = []
    for start in (0, own - halo):
        to = pl.ds(0 if start == 0 else halo, halo)
        pairs += [(ref.at[pl.ds(start, halo), :], dst.at[to, :]) for ref, dst in ((log_in, logs), (src_in, sources))]
    copies = load(sems, *pairs)
    for side in range(2):
        for copy in copies[2 * side : 2 * side + 2]:
            copy.wait()
        base = PAD + halo + side * (own - halo)
        convert([(side * halo + k, base + k) for k in range(0, halo, 8)], logs, sources, c0, s0)
    next_first, _ = towards_next()
    start = jnp.where(next_first, own - halo, 0)
    for ref, base in ((first_ref, start), (second_ref, own - halo - start)):
        for i in range(halo // 8):
            rows = pl.ds(pl.multiple_of(PAD + halo + base + 8 * i, 8), 8)
            for t in range(tiles):
                ref[t, 8 * i : 8 * i + 8, :] = c0[t, rows, :]
                ref[tiles + t, 8 * i : 8 * i + 8, :] = s0[t, rows, :]


def inner_kernel(peers, log_in, src_in, c0_in, s0_in, c0, s0, a0, bp0, va0, c1, logs, sources, sems):
    halo, own, tiles = HALO[0], OWN[0], TILES[0]
    inner = pl.ds(halo, own - 2 * halo)
    copies = load(sems, (log_in.at[inner, :], logs), (src_in.at[inner, :], sources))
    clear_pads(c0, c1, value=1.0)
    clear_pads(s0, bp0, va0)
    for copy in copies:
        copy.wait()
    convert([(k, PAD + 2 * halo + k) for k in range(0, own - 2 * halo, 8)], logs, sources, c0, s0)
    make_weights(0, c0, a0, peers, (4, 10), s0, bp0)
    restrict((2, 5), c0, PAD, range(tiles), quarter_store(c1))
    relax(0, bp0, va0, bp0, a0, (5, 9))


def scaled_store(bp_ref, a_ref, start=0):
    def store(j, k, q):
        bp_ref[start + k, at(j, PAD), :] = a_ref[4, k, at(j, 0), :] * q

    return store


def quarter_store(c_ref):
    def store(j, k, q):
        c_ref[k, at(j, PAD), :] = 0.25 * q

    return store


def open_kernel(
    peers, c0_in, s0_in, a0_in, b0_in, v0_in, c1_in, first_ref, second_ref,
    c0, s0, a0, bp0, va0, c1, msg_ref, a1, bp1, va1,
    vb0, vb1,
):
    halo, own, tiles = HALO[0], OWN[0], TILES[0]
    next_first, _ = towards_next()
    above, below = PAD, PAD + halo + own
    for ref, base in ((first_ref, jnp.where(next_first, below, above)), (second_ref, jnp.where(next_first, above, below))):
        for i in range(halo // 8):
            rows = pl.ds(pl.multiple_of(base + 8 * i, 8), 8)
            for t in range(tiles):
                c0[t, rows, :] = ref[t, 8 * i : 8 * i + 8, :]
                s0[t, rows, :] = ref[tiles + t, 8 * i : 8 * i + 8, :]
    clear_pads(vb0, bp1, va1, vb1)
    for strips in ((0, 4), (10, 14)):
        make_weights(0, c0, a0, peers, strips, s0, bp0)
    for strips in ((0, 2), (5, 7)):
        restrict(strips, c0, PAD, range(tiles), quarter_store(c1), 2)
    make_weights(1, c1, a1, peers)
    restrict(STRIPS[1], s0, PAD, range(tiles), scaled_store(bp1, a1, TILES[1]))
    for strips in ((0, 5), (9, 14)):
        relax(0, bp0, va0, bp0, a0, strips)
    residual(0, va0, vb0, bp0, a0)
    restrict(STRIPS[1], vb0, PAD, range(tiles), scaled_store(bp1, a1))
    relax(1, bp1, va1, bp1, a1)
    residual(1, va1, vb1, bp1, a1, (1, 6))

    def store(j, k, q):
        msg_ref[k, at(j, 0), :] = q

    restrict(OWN[2] // 8, vb1, PAD + HALO[1], range(2 * TILES[1]), store, 2)

    def store_coef(j, k, q):
        msg_ref[2 * TILES[2] + k, at(j, 0), :] = 0.25 * q

    restrict(OWN[2] // 8, c1, PAD + HALO[1], range(TILES[1]), store_coef, 2)


def deep_solve(a, bp, va, vb):
    relax(2, bp[2], va[2], bp[2], a[2])
    residual(2, va[2], vb[2], bp[2], a[2])
    for s in range(2):
        restrict(STRIPS[3], vb[2], PAD, range(s * 4, s * 4 + 4), scaled_store(bp[3], a[3], s * 2), 5)
    relax(3, bp[3], va[3], bp[3], a[3])
    residual(3, va[3], vb[3], bp[3], a[3])
    for s in range(2):
        restrict(STRIPS[4], vb[3], PAD, range(s * 2, s * 2 + 2), scaled_store(bp[4], a[4], s), 3)
    relax(4, bp[4], va[4], bp[4], a[4])
    relax(4, va[4], vb[4], bp[4], a[4])
    relax(4, vb[4], va[4], bp[4], a[4])
    prolong(2, va[4], PAD, range(2), va[3], unroll=2)
    relax(3, va[3], vb[3], bp[3], a[3], (0, 5))
    relax(3, vb[3], va[3], bp[3], a[3], (1, 4))
    prolong((1, 4), va[3], PAD, range(4), va[2], unroll=3)
    relax(2, va[2], vb[2], bp[2], a[2], (3, 7))
    relax(2, vb[2], va[2], bp[2], a[2], (3, 7))


def up_level_1(va2, va1, vb1, bp1, a1, strips=(0, 7)):
    offset = PAD + HALO[2] - HALO[1] // 2
    prolong(4, va2, offset, range(2 * TILES[2]), va1)
    relax(1, va1, vb1, bp1, a1, strips)
    relax(1, vb1, va1, bp1, a1, strips)


def up_level_0(va1, va0, vb0, bp0, a0, first, second):
    prolong(STRIPS[1], va1, PAD, range(TILES[1]), va0)
    relax(0, va0, vb0, bp0, a0, first)
    relax(0, vb0, va0, bp0, a0, second)


def assemble(messages, a2, bp2):
    for position, m in zip(slab_positions(), messages):
        for i in range(2):
            row = pl.multiple_of(position * OWN[2] + i * 8, 8)
            for k in range(2 * TILES[2]):
                bp2[k, pl.ds(PAD + row, 8), :] = (
                    a2[4, k % TILES[2], pl.ds(row, 8), :] * m[k, i * 8 : i * 8 + 8, :]
                )


def middle_kernel(
    peers, m0, m1, m2, m3, m4, a0, bp0, va0_in, a1, bp1_in, va1_in,
    msg_ref, a2, a3, a4, va0, bp1, va1,
    vb0, vb1, c2, bp2, va2, vb2, c3, bp3, va3, vb3, c4, bp4, va4, vb4,
):
    messages = (m0, m1, m2, m3, m4)
    fill(c4, 1.0)
    clear_pads(c2, c3, value=1.0)
    for ref in (bp4, va4, vb4):
        fill(ref, 0.0)
    clear_pads(bp2, va2, vb2, bp3, va3, vb3)
    clear_pads(vb0, vb1, size=2 * PAD)
    for position, m in zip(slab_positions(), messages):
        for i in range(2):
            row = pl.multiple_of(position * OWN[2] + i * 8, 8)
            for k in range(TILES[2]):
                c2[k, pl.ds(PAD + row, 8), :] = m[2 * TILES[2] + k, i * 8 : i * 8 + 8, :]
    make_weights(2, c2, a2, peers)
    restrict(STRIPS[3], c2, PAD, range(4), quarter_store(c3), 5)
    make_weights(3, c3, a3, peers)
    restrict(2, c3, PAD, range(2), quarter_store(c4), 2)

    def last_rows(j, k, q):
        c4[k, PAD + 16 : PAD + 24, :] = jnp.where(iota(0) < ROWS[4] - 16, 0.25 * q, 1.0)

    restrict(1, c3, PAD + 32, range(2), last_rows)
    make_weights(4, c4, a4, peers)
    assemble(messages, a2, bp2)
    a = {2: a2, 3: a3, 4: a4}
    bp = {2: bp2, 3: bp3, 4: bp4}
    va = {2: va2, 3: va3, 4: va4}
    vb = {2: vb2, 3: vb3, 4: vb4}
    deep_solve(a, bp, va, vb)
    up_level_1(va2, va1, vb1, bp1, a1)
    up_level_0(va1, va0, vb0, bp0, a0, (1, 13), (1, 13))

    relax(0, va0, vb0, bp0, a0, (1, 13))
    relax(0, vb0, va0, bp0, a0, (1, 13))
    residual(0, va0, vb0, bp0, a0, (1, 13))
    restrict((1, 6), vb0, PAD, range(TILES[0]), scaled_store(bp1, a1))

    def clear(i):
        va1[0 : TILES[1], at(i, 0), :] = jnp.zeros((TILES[1], 8, LANES), F32)

    loop(BUF[1] // 8, clear)
    relax(1, va1, vb1, bp1, a1)
    relax(1, vb1, va1, bp1, a1)
    residual(1, va1, vb1, bp1, a1, (1, 6))

    def store(j, k, q):
        msg_ref[k, at(j, 0), :] = q

    restrict(OWN[2] // 8, vb1, PAD + HALO[1], range(2 * TILES[1]), store, 2)


def close_kernel(
    m0, m1, m2, m3, m4, a0, bp0, va0_in, a1, bp1, va1_in, a2, a3, a4,
    va0, va1, out_hbm, mine_ref, other_ref,
    vb0, vb1, bp2, va2, vb2, bp3, va3, vb3, bp4, va4, vb4, out_ref, sems,
):
    for ref in (bp4, va4, vb4):
        fill(ref, 0.0)
    clear_pads(bp2, va2, vb2, bp3, va3, vb3)
    clear_pads(vb0, vb1, size=2 * PAD)
    assemble((m0, m1, m2, m3, m4), a2, bp2)
    a = {2: a2, 3: a3, 4: a4}
    bp = {2: bp2, 3: bp3, 4: bp4}
    va = {2: va2, 3: va3, 4: va4}
    vb = {2: vb2, 3: vb3, 4: vb4}
    deep_solve(a, bp, va, vb)
    up_level_1(va2, va1, vb1, bp1, a1, (1, 6))
    up_level_0(va1, va0, vb0, bp0, a0, (2, 12), (3, 11))
    prolong(OWN[1] // 8, va1, PAD + HALO[1], range(TILES[1], 2 * TILES[1]), va0, -1.0, PAD + HALO[0])
    tiles = TILES[0]
    left = lax.axis_index("samp") == 0

    copies = []
    for piece in range(OWN[0] // 16):
        strips = (2 * piece, 2 * piece + 1)
        turned = turn([[va0[t, at(j, PAD + HALO[0]), :] for t in range(tiles)] for j in strips])
        for j, x in zip(strips, turned):
            for t in range(tiles):
                out_ref[at(j, 0), t * LANES : (t + 1) * LANES] = x[t]
            for t in range(tiles // 2):
                low, high = x[t], x[tiles // 2 + t]
                mine_ref[at(j, 0), t * LANES : (t + 1) * LANES] = jnp.where(left, low, high)
                other_ref[at(j, 0), t * LANES : (t + 1) * LANES] = jnp.where(left, high, low)
        rows = pl.ds(16 * piece, 16)
        copies.append(pltpu.make_async_copy(out_ref.at[rows, :], out_hbm.at[rows, :], sems.at[piece]))
        copies[-1].start()
    for copy in copies:
        copy.wait()


VMEM = pl.BlockSpec(memory_space=pltpu.VMEM)


def near(*dims):
    return pltpu.VMEM(dims, F32)


def held(*values):
    return [pltpu.with_memory_space_constraint(v, pltpu.VMEM) for v in values]


def a_shape(level):
    return (6, TILES[level], 8 * STRIPS[level], LANES)


def v_shape(level):
    return (SOLVES[level] * TILES[level], BUF[level], LANES)


def c_shape(level):
    return (TILES[level], BUF[level], LANES)


FAR = pl.BlockSpec(memory_space=pltpu.HBM)


def call(kernel, name, arguments, outputs, scratch=(), aliases=None, sems=0, far=0):
    return pl.pallas_call(
        kernel,
        out_shape=outputs,
        in_specs=[FAR] * far + [VMEM] * (len(arguments) - far),
        out_specs=[FAR if isinstance(o, jax.ShapeDtypeStruct) else VMEM for o in outputs],
        scratch_shapes=[pltpu.VMEM(s, F32) for s in scratch] + ([pltpu.SemaphoreType.DMA((sems,))] if sems else []),
        input_output_aliases=aliases or {},
        compiler_params=pltpu.CompilerParams(vmem_limit_bytes=24 * 2**20),
        cost_estimate=pl.CostEstimate(flops=10**8, bytes_accessed=10**6, transcendentals=0),
        name=name,
    )(*arguments)


def swaps(distance):
    peers = lax.axis_size("grid")
    even = [(i, i + distance if i % (2 * distance) < distance else i - distance) for i in range(peers)]
    odd = [(a + distance, b + distance) for a, b in even if max(a, b) + distance < peers]
    last = peers - 1
    odd += [(0, last), (last, 0)] if distance == 1 else [(0, 1), (1, 0), (last - 1, last), (last, last - 1)]
    return even, odd


def gathered(value):
    return [lax.ppermute(value, "grid", pairs) for distance in (1, 2) for pairs in swaps(distance)] + [value]


def local(log_coef, source):
    peers = lax.axis_size("grid")
    log_field, source_field = log_coef[0], source[0]
    rows, columns = source_field.shape
    edge = near(2 * TILES[0], HALO[0], LANES)
    fields = [pltpu.with_memory_space_constraint(x, pltpu.HBM) for x in (log_field, source_field)]
    c0, s0, first, second = call(
        pack_kernel, "pack", fields, (near(*c_shape(0)), near(*c_shape(0)), edge, edge),
        [(2 * HALO[0], columns)] * 2, sems=4, far=2,
    )
    even, odd = swaps(1)
    first, second = lax.ppermute(first, "grid", even), lax.ppermute(second, "grid", odd)

    state = [near(*f(level)) for level in (0, 1) for f in (a_shape, v_shape, v_shape)]
    whole = [near(*c_shape(0)), near(*c_shape(0))] + state[:3] + [near(*c_shape(1))]
    middle_rows = rows - 2 * HALO[0]
    started = call(
        functools.partial(inner_kernel, peers), "inner", [*fields, *held(c0, s0)], whole,
        [(middle_rows, columns)] * 2, {2: 0, 3: 1}, sems=2, far=2,
    )
    c0, s0, a0, b0, v0, c1, message, a1, b1, v1 = call(
        functools.partial(open_kernel, peers),
        "open",
        held(*started, first, second),
        whole + [near(3 * TILES[2], OWN[2], LANES)] + state[3:],
        [v_shape(0), v_shape(1)],
        {k: k for k in range(6)},
    )
    deep = [shape for level in (2, 3, 4) for shape in [c_shape(level)] + [v_shape(level)] * 3]
    message, a2, a3, a4, v0, b1, v1 = call(
        functools.partial(middle_kernel, peers),
        "middle",
        held(*gathered(message), a0, b0, v0, a1, b1, v1),
        [near(2 * TILES[2], OWN[2], LANES)] + [near(*a_shape(level)) for level in (2, 3, 4)] + [state[k] for k in (2, 4, 5)],
        [v_shape(0), v_shape(1)] + deep,
        {7: 4, 9: 5, 10: 6},
    )
    deep = [shape for level in (2, 3, 4) for shape in [v_shape(level)] * 3]
    half = near(rows, columns // 2)
    v0, v1, correction, mine, other = call(
        close_kernel,
        "close",
        held(*gathered(message), a0, b0, v0, a1, b1, v1, a2, a3, a4),
        (state[2], state[5], jax.ShapeDtypeStruct((rows, columns), F32), half, half),
        [v_shape(0), v_shape(1)] + deep + [(rows, columns)],
        {7: 0, 10: 1},
        sems=rows // 16,
    )

    theirs = lax.ppermute(other, "samp", [(0, 1), (1, 0)])
    samples = lax.axis_size("samp")
    level_mean = (mine + theirs) / samples
    squares = mine * mine + theirs * theirs
    level_var = (squares - samples * level_mean * level_mean) / (samples - 1)
    return (correction[None], level_mean, level_var)


def solution(mesh):
    in_specs = (P("samp", "grid", None), P("samp", "grid", None))
    out_specs = (P("samp", "grid", None), P("grid", "samp"), P("grid", "samp"))
    return jax.shard_map(local, mesh=mesh, in_specs=in_specs, out_specs=out_specs, check_vma=False)
```

```python
import functools

import jax
import jax.numpy as jnp
from jax import lax
from jax.experimental import pallas as pl
from jax.experimental.pallas import tpu as pltpu
from jax.sharding import PartitionSpec as P


LANES = 128
PAD = 8
OWN = (64, 32, 16, 8, 4)
HALO = (24, 12, 32, 16, 8)
ROWS = tuple(o + 2 * h for o, h in zip(OWN, HALO))
TILES = (16, 8, 4, 2, 1)
STRIPS = (14, 7, 10, 5, 3)
BUF = tuple(8 * s + 2 * PAD for s in STRIPS)
SOLVES = (1, 2, 2, 2, 2)
UNROLL = (2, 7, 5, 5, 3)
DAMP = 0.8
NEAR = 8
F32 = jnp.float32


def loop(count, body, unroll=1):
    first, last = count if isinstance(count, tuple) else (0, count)
    if unroll >= last - first:
        for i in range(first, last):
            body(i)
    else:
        lax.fori_loop(first, last, lambda i, c: (body(i), c)[1], 0, unroll=unroll)


def at(i, offset, step=8):
    if isinstance(i, int):
        return pl.ds(i * step + offset, 8)
    return pl.ds(pl.multiple_of(i * step, step) + offset, 8)


def pairs_at(i, offset):
    base = i * 16 if isinstance(i, int) else pl.multiple_of(i * 16, 16)
    return pl.ds(base + offset, 8, stride=2), pl.ds(base + offset + 1, 8, stride=2)


def iota(dim):
    return lax.broadcasted_iota(jnp.int32, (8, LANES), dim)


def from_west(x):
    return jnp.where(iota(1) < 16, pltpu.roll(x, 17, 1), pltpu.roll(x, 16, 1))


def from_east(x):
    return jnp.where(iota(1) >= LANES - 16, pltpu.roll(x, LANES - 17, 1), pltpu.roll(x, LANES - 16, 1))


def side_values(x):
    return [from_west(x[-1])] + x[:-1], x[1:] + [from_east(x[0])]


def harmonic(a, b):
    return 2.0 * a * b / (a + b)


def make_weights(level, c_ref, a_ref, peers, strips=None, source_ref=None, b_ref=None):
    tiles = TILES[level]
    top, total_rows = first_row(level), peers * OWN[level]

    def body(i):
        c = [c_ref[t, at(i, PAD), :] for t in range(tiles)]
        row = top + i * 8 + iota(0)
        lane = iota(1)
        inside = jnp.logical_and(row >= 0, row < total_rows)
        west, east = side_values(c)
        west[0] = jnp.where(lane == 0, c[0], west[0])
        east[-1] = jnp.where(lane == LANES - 1, c[-1], east[-1])
        w_east = [harmonic(a, b) for a, b in zip(c, east)]
        w_west = [harmonic(c[0], west[0])] + w_east[:-1]
        for t in range(tiles):
            w_north = harmonic(c[t], jnp.where(row == 0, c[t], c_ref[t, at(i, PAD - 1), :]))
            w_south = harmonic(c[t], jnp.where(row == total_rows - 1, c[t], c_ref[t, at(i, PAD + 1), :]))
            diagonal = w_west[t] + w_east[t] + w_north + w_south
            gain = jnp.where(inside, DAMP / diagonal, 0.0)
            a_west, a_east = gain * w_west[t], gain * w_east[t]
            if t == 0:
                a_west = jnp.where(lane == 0, 0.0, a_west)
            if t == tiles - 1:
                a_east = jnp.where(lane == LANES - 1, 0.0, a_east)
            rows = at(i, 0)
            a_ref[0, t, rows, :] = a_west
            a_ref[1, t, rows, :] = a_east
            a_ref[2, t, rows, :] = gain * w_north
            a_ref[3, t, rows, :] = gain * w_south
            a_ref[4, t, rows, :] = gain
            a_ref[5, t, rows, :] = diagonal * (1.0 / DAMP)
            if source_ref is not None:
                b_ref[t, at(i, PAD), :] = gain * source_ref[t, at(i, PAD), :]

    loop(strips or STRIPS[level], body, UNROLL[level])


def sweep(level, v_ref, out_ref, b_ref, a_ref, finish, strips):
    tiles, solves = TILES[level], SOLVES[level]

    def body(i):
        v = [[v_ref[s * tiles + t, at(i, PAD), :] for t in range(tiles)] for s in range(solves)]
        sides = [side_values(x) for x in v]
        rows = at(i, 0)
        order = list(range(1, tiles - 1)) + ([0, tiles - 1] if tiles > 1 else [0])
        for t in order:
            a_west, a_east, a_north, a_south = (a_ref[k, t, rows, :] for k in range(4))
            for s in range(solves):
                west, east = sides[s]
                k = s * tiles + t
                north, south = v_ref[k, at(i, PAD - 1), :], v_ref[k, at(i, PAD + 1), :]
                moved = (a_north * north + a_south * south) + b_ref[k, at(i, PAD), :]
                moved += a_west * west[t] + a_east * east[t]
                out_ref[k, at(i, PAD), :] = finish(v[s][t], moved, t, rows)

    loop(strips or STRIPS[level], body, UNROLL[level])


def relax(level, v_ref, out_ref, b_ref, a_ref, strips=None):
    sweep(level, v_ref, out_ref, b_ref, a_ref, lambda v, moved, t, rows: (1.0 - DAMP) * v + moved, strips)


def residual(level, v_ref, out_ref, b_ref, a_ref, strips=None):
    def finish(v, moved, t, rows):
        return a_ref[5, t, rows, :] * (moved - DAMP * v)

    sweep(level, v_ref, out_ref, b_ref, a_ref, finish, strips)


def restrict(count, ref, offset, tiles, store, unroll=1):
    def body(j):
        even, odd = pairs_at(j, offset)
        for k in range(0, len(tiles), 2):
            a, b = tiles[k], tiles[k + 1]
            store(j, k // 2, (ref[a, even, :] + ref[a, odd, :]) + (ref[b, even, :] + ref[b, odd, :]))

    loop(count, body, unroll)


def prolong(count, e_ref, offset, e_tiles, v_ref, sign=1.0, v_offset=PAD, unroll=1):
    def body(j):
        halves = pairs_at(j, v_offset)
        for k, tile in enumerate(e_tiles):
            e = sign * e_ref[tile, at(j, offset), :]
            for t in (2 * k, 2 * k + 1):
                for rows in halves:
                    v_ref[t, rows, :] = v_ref[t, rows, :] + e

    loop(count, body, unroll)


def clear_pads(*refs, value=0.0, size=PAD):
    for ref in refs:
        tiles, rows, _ = ref.shape
        ref[:, 0:size, :] = jnp.full((tiles, size, LANES), value, F32)
        ref[:, rows - size : rows, :] = jnp.full((tiles, size, LANES), value, F32)


def fill(ref, value):
    def body(i):
        ref[:, at(i, 0), :] = jnp.full((ref.shape[0], 8, LANES), value, F32)

    loop(ref.shape[1] // 8, body)


def turn(groups):
    lane = iota(1)
    groups = [list(x) for x in groups]
    for step in (1, 2, 4, 8):
        upper = lax.rem(lane, 2 * step) >= step
        for i in range(16):
            if i & step == 0:
                j = i + step
                for x in groups:
                    from_j = pltpu.roll(x[j], step, 1)
                    from_i = pltpu.roll(x[i], LANES - step, 1)
                    x[i], x[j] = jnp.where(upper, from_j, x[i]), jnp.where(upper, x[j], from_i)
    return groups


def place():
    return lax.axis_index("grid")


def first_row(level):
    return place() * OWN[level] - HALO[level]


def towards_next():
    i = place()
    return lax.rem(i, 2) == 0, lax.rem(i, 4) < 2


def slab_positions():
    next_first, far = towards_next()
    return (
        jnp.where(next_first, 3, 1), jnp.where(next_first, 1, 3), jnp.where(far, 4, 0), jnp.where(far, 0, 4), 2,
    )


def convert(rows_of, log_ref, src_ref, c0, s0):
    tiles = TILES[0]
    for row, to in rows_of:
        logs, sources = ([ref[row : row + 8, t * LANES : (t + 1) * LANES] for t in range(tiles)] for ref in (log_ref, src_ref))
        for ref, x in zip((c0, s0), turn(([jnp.exp(v) for v in logs], sources))):
            for t, v in enumerate(x):
                ref[t, to : to + 8, :] = v


def load(sems, *pairs):
    copies = [pltpu.make_async_copy(src, dst, sems.at[k]) for k, (src, dst) in enumerate(pairs)]
    for copy in copies:
        copy.start()
    return copies


def boundary_rows(near):
    count = NEAR if near else HALO[0] - NEAR
    start = 0 if near else NEAR
    return (start, count), (OWN[0] - start - count, count)


def pack_kernel(near, log_in, src_in, *refs):
    c0, s0, first_ref, second_ref, logs, sources, sems = refs if near else refs[2:]
    tiles = TILES[0]
    sides = boundary_rows(near)
    count = sides[0][1]
    pairs = []
    for side, (start, _) in enumerate(sides):
        to = pl.ds(side * count, count)
        pairs += [(ref.at[pl.ds(start, count), :], dst.at[to, :]) for ref, dst in ((log_in, logs), (src_in, sources))]
    copies = load(sems, *pairs)
    for side, (start, _) in enumerate(sides):
        for copy in copies[2 * side : 2 * side + 2]:
            copy.wait()
        base = PAD + HALO[0] + start
        convert([(side * count + k, base + k) for k in range(0, count, 8)], logs, sources, c0, s0)
    next_first, _ = towards_next()
    up, down = (PAD + HALO[0] + start for start, _ in sides)
    for ref, base in ((first_ref, jnp.where(next_first, down, up)), (second_ref, jnp.where(next_first, up, down))):
        for i in range(count // 8):
            rows = pl.ds(pl.multiple_of(base + 8 * i, 8), 8)
            for t in range(tiles):
                ref[t, 8 * i : 8 * i + 8, :] = c0[t, rows, :]
                ref[tiles + t, 8 * i : 8 * i + 8, :] = s0[t, rows, :]


def inner_kernel(peers, log_in, src_in, c0_in, s0_in, c0, s0, a0, bp0, va0, c1, logs, sources, sems):
    halo, own, tiles = HALO[0], OWN[0], TILES[0]
    inner = pl.ds(halo, own - 2 * halo)
    copies = load(sems, (log_in.at[inner, :], logs), (src_in.at[inner, :], sources))
    clear_pads(c0, value=1.0, size=PAD + halo)
    clear_pads(s0, bp0, va0, size=PAD + halo)
    clear_pads(c1, value=1.0)
    for copy in copies:
        copy.wait()
    convert([(k, PAD + 2 * halo + k) for k in range(0, own - 2 * halo, 8)], logs, sources, c0, s0)
    make_weights(0, c0, a0, peers, (4, 10), s0, bp0)
    restrict((2, 5), c0, PAD, range(tiles), quarter_store(c1))
    relax(0, bp0, va0, bp0, a0, (5, 9))


def insert(first_ref, second_ref, near, c0, s0):
    tiles = TILES[0]
    next_first, _ = towards_next()
    count = first_ref.shape[1]
    above = PAD + (HALO[0] - NEAR if near else 0)
    below = PAD + HALO[0] + OWN[0] + (0 if near else NEAR)
    for ref, base in ((first_ref, jnp.where(next_first, below, above)), (second_ref, jnp.where(next_first, above, below))):
        for i in range(count // 8):
            rows = pl.ds(pl.multiple_of(base + 8 * i, 8), 8)
            for t in range(tiles):
                c0[t, rows, :] = ref[t, 8 * i : 8 * i + 8, :]
                s0[t, rows, :] = ref[tiles + t, 8 * i : 8 * i + 8, :]


def scaled_store(bp_ref, a_ref, start=0):
    def store(j, k, q):
        bp_ref[start + k, at(j, PAD), :] = a_ref[4, k, at(j, 0), :] * q

    return store


def quarter_store(c_ref):
    def store(j, k, q):
        c_ref[k, at(j, PAD), :] = 0.25 * q

    return store


def outer_kernel(peers, *refs):
    first_ref, second_ref = refs[9:11]
    c0, s0, a0, bp0, va0, c1, a1, bp1, va1, vb0 = refs[11:]
    tiles = TILES[0]
    insert(first_ref, second_ref, False, c0, s0)
    clear_pads(vb0)
    ends = ((0, 2), (5, 7))
    for strips in ((0, 3), (11, 14)):
        make_weights(0, c0, a0, peers, strips, s0, bp0)
    for strips in ends:
        restrict(strips, c0, PAD, range(tiles), quarter_store(c1), 2)
    for strips in ends:
        make_weights(1, c1, a1, peers, strips)
        restrict(strips, s0, PAD, range(tiles), scaled_store(bp1, a1, TILES[1]), 2)
    for strips in ((0, 4), (10, 14)):
        relax(0, bp0, va0, bp0, a0, strips)
    for strips in ((0, 4), (10, 14)):
        residual(0, va0, vb0, bp0, a0, strips)
    for strips in ends:
        restrict(strips, vb0, PAD, range(tiles), scaled_store(bp1, a1), 2)
    relax(1, bp1, va1, bp1, a1)


def open_kernel(
    peers, c0_in, s0_in, a0_in, b0_in, v0_in, c1_in, first_ref, second_ref,
    c0, s0, a0, bp0, va0, c1, a1, bp1, va1, msg_ref,
    vb0, vb1,
):
    tiles = TILES[0]
    insert(first_ref, second_ref, True, c0, s0)
    clear_pads(va1, vb1, size=2 * PAD)
    clear_pads(bp1, size=2 * PAD)
    for strips in ((2, 4), (10, 12)):
        make_weights(0, c0, a0, peers, strips, s0, bp0)
    for strips in ((1, 2), (5, 6)):
        restrict(strips, c0, PAD, range(tiles), quarter_store(c1), 2)
    make_weights(1, c1, a1, peers, (1, 6))
    restrict((1, 6), s0, PAD, range(tiles), scaled_store(bp1, a1, TILES[1]))
    for strips in ((2, 5), (9, 12)):
        relax(0, bp0, va0, bp0, a0, strips)
    residual(0, va0, vb0, bp0, a0, (2, 12))
    restrict((1, 6), vb0, PAD, range(tiles), scaled_store(bp1, a1))
    relax(1, bp1, va1, bp1, a1, (1, 6))
    residual(1, va1, vb1, bp1, a1, (1, 6))

    def store(j, k, q):
        msg_ref[k, at(j, 0), :] = q

    restrict(OWN[2] // 8, vb1, PAD + HALO[1], range(2 * TILES[1]), store, 2)

    def store_coef(j, k, q):
        msg_ref[2 * TILES[2] + k, at(j, 0), :] = 0.25 * q

    restrict(OWN[2] // 8, c1, PAD + HALO[1], range(TILES[1]), store_coef, 2)


def deep_solve(a, bp, va, vb):
    relax(2, bp[2], va[2], bp[2], a[2])
    residual(2, va[2], vb[2], bp[2], a[2])
    for s in range(2):
        restrict(STRIPS[3], vb[2], PAD, range(s * 4, s * 4 + 4), scaled_store(bp[3], a[3], s * 2), 5)
    relax(3, bp[3], va[3], bp[3], a[3])
    residual(3, va[3], vb[3], bp[3], a[3])
    for s in range(2):
        restrict(STRIPS[4], vb[3], PAD, range(s * 2, s * 2 + 2), scaled_store(bp[4], a[4], s), 3)
    relax(4, bp[4], va[4], bp[4], a[4])
    relax(4, va[4], vb[4], bp[4], a[4])
    relax(4, vb[4], va[4], bp[4], a[4])
    prolong(2, va[4], PAD, range(2), va[3], unroll=2)
    relax(3, va[3], vb[3], bp[3], a[3], (0, 5))
    relax(3, vb[3], va[3], bp[3], a[3], (1, 4))
    prolong((1, 4), va[3], PAD, range(4), va[2], unroll=3)
    relax(2, va[2], vb[2], bp[2], a[2], (3, 7))
    relax(2, vb[2], va[2], bp[2], a[2], (3, 7))


def up_level_1(va2, va1, vb1, bp1, a1, strips=(0, 7)):
    offset = PAD + HALO[2] - HALO[1] // 2
    prolong(4, va2, offset, range(2 * TILES[2]), va1)
    relax(1, va1, vb1, bp1, a1, strips)
    relax(1, vb1, va1, bp1, a1, strips)


def up_level_0(va1, va0, vb0, bp0, a0, first, second):
    prolong(STRIPS[1], va1, PAD, range(TILES[1]), va0)
    relax(0, va0, vb0, bp0, a0, first)
    relax(0, vb0, va0, bp0, a0, second)


def assemble(messages, a2, bp2):
    for position, m in zip(slab_positions(), messages):
        for i in range(2):
            row = pl.multiple_of(position * OWN[2] + i * 8, 8)
            for k in range(2 * TILES[2]):
                bp2[k, pl.ds(PAD + row, 8), :] = (
                    a2[4, k % TILES[2], pl.ds(row, 8), :] * m[k, i * 8 : i * 8 + 8, :]
                )


def middle_kernel(
    peers, m0, m1, m2, m3, m4, a0, bp0, va0_in, a1, bp1_in, va1_in,
    msg_ref, a2, a3, a4, va0, bp1, va1,
    vb0, vb1, c2, bp2, va2, vb2, c3, bp3, va3, vb3, c4, bp4, va4, vb4,
):
    messages = (m0, m1, m2, m3, m4)
    fill(c4, 1.0)
    clear_pads(c2, c3, value=1.0)
    for ref in (bp4, va4, vb4):
        fill(ref, 0.0)
    clear_pads(bp2, va2, vb2, bp3, va3, vb3)
    clear_pads(vb0, vb1, size=2 * PAD)
    for position, m in zip(slab_positions(), messages):
        for i in range(2):
            row = pl.multiple_of(position * OWN[2] + i * 8, 8)
            for k in range(TILES[2]):
                c2[k, pl.ds(PAD + row, 8), :] = m[2 * TILES[2] + k, i * 8 : i * 8 + 8, :]
    make_weights(2, c2, a2, peers)
    restrict(STRIPS[3], c2, PAD, range(4), quarter_store(c3), 5)
    make_weights(3, c3, a3, peers)
    restrict(2, c3, PAD, range(2), quarter_store(c4), 2)

    def last_rows(j, k, q):
        c4[k, PAD + 16 : PAD + 24, :] = jnp.where(iota(0) < ROWS[4] - 16, 0.25 * q, 1.0)

    restrict(1, c3, PAD + 32, range(2), last_rows)
    make_weights(4, c4, a4, peers)
    assemble(messages, a2, bp2)
    a = {2: a2, 3: a3, 4: a4}
    bp = {2: bp2, 3: bp3, 4: bp4}
    va = {2: va2, 3: va3, 4: va4}
    vb = {2: vb2, 3: vb3, 4: vb4}
    deep_solve(a, bp, va, vb)
    up_level_1(va2, va1, vb1, bp1, a1)
    up_level_0(va1, va0, vb0, bp0, a0, (1, 13), (1, 13))

    relax(0, va0, vb0, bp0, a0, (1, 13))
    relax(0, vb0, va0, bp0, a0, (1, 13))
    residual(0, va0, vb0, bp0, a0, (1, 13))
    restrict((1, 6), vb0, PAD, range(TILES[0]), scaled_store(bp1, a1))

    def clear(i):
        va1[0 : TILES[1], at(i, 0), :] = jnp.zeros((TILES[1], 8, LANES), F32)

    loop(BUF[1] // 8, clear)
    relax(1, va1, vb1, bp1, a1)
    relax(1, vb1, va1, bp1, a1)
    residual(1, va1, vb1, bp1, a1, (1, 6))

    def store(j, k, q):
        msg_ref[k, at(j, 0), :] = q

    restrict(OWN[2] // 8, vb1, PAD + HALO[1], range(2 * TILES[1]), store, 2)


def close_kernel(
    m0, m1, m2, m3, m4, a0, bp0, va0_in, a1, bp1, va1_in, a2, a3, a4,
    va0, va1, out_hbm, mine_ref, other_ref,
    vb0, vb1, bp2, va2, vb2, bp3, va3, vb3, bp4, va4, vb4, out_ref, sems,
):
    for ref in (bp4, va4, vb4):
        fill(ref, 0.0)
    clear_pads(bp2, va2, vb2, bp3, va3, vb3)
    clear_pads(vb0, vb1, size=2 * PAD)
    assemble((m0, m1, m2, m3, m4), a2, bp2)
    a = {2: a2, 3: a3, 4: a4}
    bp = {2: bp2, 3: bp3, 4: bp4}
    va = {2: va2, 3: va3, 4: va4}
    vb = {2: vb2, 3: vb3, 4: vb4}
    deep_solve(a, bp, va, vb)
    up_level_1(va2, va1, vb1, bp1, a1, (1, 6))
    up_level_0(va1, va0, vb0, bp0, a0, (2, 12), (3, 11))
    prolong(OWN[1] // 8, va1, PAD + HALO[1], range(TILES[1], 2 * TILES[1]), va0, -1.0, PAD + HALO[0])
    tiles = TILES[0]
    left = lax.axis_index("samp") == 0

    copies = []
    for piece in range(OWN[0] // 16):
        strips = (2 * piece, 2 * piece + 1)
        turned = turn([[va0[t, at(j, PAD + HALO[0]), :] for t in range(tiles)] for j in strips])
        for j, x in zip(strips, turned):
            for t in range(tiles):
                out_ref[at(j, 0), t * LANES : (t + 1) * LANES] = x[t]
            for t in range(tiles // 2):
                low, high = x[t], x[tiles // 2 + t]
                mine_ref[at(j, 0), t * LANES : (t + 1) * LANES] = jnp.where(left, low, high)
                other_ref[at(j, 0), t * LANES : (t + 1) * LANES] = jnp.where(left, high, low)
        rows = pl.ds(16 * piece, 16)
        copies.append(pltpu.make_async_copy(out_ref.at[rows, :], out_hbm.at[rows, :], sems.at[piece]))
        copies[-1].start()
    for copy in copies:
        copy.wait()


VMEM = pl.BlockSpec(memory_space=pltpu.VMEM)


def near(*dims):
    return pltpu.VMEM(dims, F32)


def held(*values):
    return [pltpu.with_memory_space_constraint(v, pltpu.VMEM) for v in values]


def a_shape(level):
    return (6, TILES[level], 8 * STRIPS[level], LANES)


def v_shape(level):
    return (SOLVES[level] * TILES[level], BUF[level], LANES)


def c_shape(level):
    return (TILES[level], BUF[level], LANES)


FAR = pl.BlockSpec(memory_space=pltpu.HBM)


def call(kernel, arguments, outputs, scratch=(), aliases=None, sems=0, far=0):
    return pl.pallas_call(
        kernel,
        out_shape=outputs,
        in_specs=[FAR] * far + [VMEM] * (len(arguments) - far),
        out_specs=[FAR if isinstance(o, jax.ShapeDtypeStruct) else VMEM for o in outputs],
        scratch_shapes=[pltpu.VMEM(s, F32) for s in scratch] + ([pltpu.SemaphoreType.DMA((sems,))] if sems else []),
        input_output_aliases=aliases or {},
        compiler_params=pltpu.CompilerParams(vmem_limit_bytes=24 * 2**20),
        cost_estimate=pl.CostEstimate(flops=10**8, bytes_accessed=10**6, transcendentals=0),
    )(*arguments)


def swaps(distance):
    peers, samples = lax.axis_size("grid"), lax.axis_size("samp")
    even = [(i, i + distance if i % (2 * distance) < distance else i - distance) for i in range(peers)]
    odd = [(a + distance, b + distance) for a, b in even if max(a, b) + distance < peers]
    ends = sorted(set(range(peers)) - {a for a, _ in odd})
    both = [[(s * peers + a, s * peers + b) for s in range(samples) for a, b in pairs] for pairs in (even, odd)]
    both[1] += [(s * peers + e, (s + 1) % samples * peers + e) for s in range(samples) for e in ends]
    return both


def swapped(value, pairs):
    return lax.ppermute(value, ("samp", "grid"), pairs)


def gathered(value):
    sets = [pairs for distance in (1, 2) for pairs in swaps(distance)]
    return [swapped(value, pairs) for pairs in sets] + [value]


def local(log_coef, source):
    peers = lax.axis_size("grid")
    log_field, source_field = log_coef[0], source[0]
    rows, columns = source_field.shape
    fields = [pltpu.with_memory_space_constraint(x, pltpu.HBM) for x in (log_field, source_field)]
    tiled = [near(*c_shape(0)), near(*c_shape(0))]
    even, odd = swaps(1)

    def send_rows(first_part, held_fields):
        count = boundary_rows(first_part)[0][1]
        edge = near(2 * TILES[0], count, LANES)
        c0, s0, first, second = call(
            functools.partial(pack_kernel, first_part), fields + held_fields,
            tiled + [edge, edge], [(2 * count, columns)] * 2, {} if first_part else {2: 0, 3: 1}, sems=4, far=2,
        )
        return [c0, s0], [swapped(first, even), swapped(second, odd)]

    tiles, first_rows = send_rows(True, [])
    tiles, rest_rows = send_rows(False, held(*tiles))
    state = [near(*f(level)) for level in (0, 1) for f in (a_shape, v_shape, v_shape)]
    whole = tiled + state[:3] + [near(*c_shape(1))]
    middle_rows = rows - 2 * HALO[0]
    started = call(
        functools.partial(inner_kernel, peers), fields + held(*tiles), whole,
        [(middle_rows, columns)] * 2, {2: 0, 3: 1}, sems=2, far=2,
    )
    *opened, message = call(
        functools.partial(open_kernel, peers), held(*started, *first_rows),
        whole + state[3:] + [near(3 * TILES[2], OWN[2], LANES)],
        [v_shape(0), v_shape(1)], {k: k for k in range(6)},
    )
    arrived = gathered(message)
    _, _, a0, b0, v0, _, a1, b1, v1 = call(
        functools.partial(outer_kernel, peers), held(*opened, *rest_rows),
        whole + state[3:], [v_shape(0)], {k: k for k in range(9)},
    )
    deep = [shape for level in (2, 3, 4) for shape in [c_shape(level)] + [v_shape(level)] * 3]
    message, a2, a3, a4, v0, b1, v1 = call(
        functools.partial(middle_kernel, peers),
        held(*arrived, a0, b0, v0, a1, b1, v1),
        [near(2 * TILES[2], OWN[2], LANES)] + [near(*a_shape(level)) for level in (2, 3, 4)] + [state[k] for k in (2, 4, 5)],
        [v_shape(0), v_shape(1)] + deep,
        {7: 4, 9: 5, 10: 6},
    )
    deep = [shape for level in (2, 3, 4) for shape in [v_shape(level)] * 3]
    half = near(rows, columns // 2)
    v0, v1, correction, mine, other = call(
        close_kernel,
        held(*gathered(message), a0, b0, v0, a1, b1, v1, a2, a3, a4),
        (state[2], state[5], jax.ShapeDtypeStruct((rows, columns), F32), half, half),
        [v_shape(0), v_shape(1)] + deep + [(rows, columns)],
        {7: 0, 10: 1},
        sems=rows // 16,
    )

    theirs = lax.ppermute(other, "samp", [(0, 1), (1, 0)])
    samples = lax.axis_size("samp")
    level_mean = (mine + theirs) / samples
    squares = mine * mine + theirs * theirs
    level_var = (squares - samples * level_mean * level_mean) / (samples - 1)
    return (correction[None], level_mean, level_var)


def solution(mesh):
    in_specs = (P("samp", "grid", None), P("samp", "grid", None))
    out_specs = (P("samp", "grid", None), P("grid", "samp"), P("grid", "samp"))
    return jax.shard_map(local, mesh=mesh, in_specs=in_specs, out_specs=out_specs, check_vma=False)
```

```python
import functools

import jax
import jax.numpy as jnp
from jax import lax
from jax.experimental import pallas as pl
from jax.experimental.pallas import tpu as pltpu
from jax.sharding import PartitionSpec as P


LANES = 128
PAD = 8
OWN = (64, 32, 16, 8, 4)
HALO = (24, 12, 32, 16, 8)
ROWS = tuple(o + 2 * h for o, h in zip(OWN, HALO))
TILES = (16, 8, 4, 2, 1)
STRIPS = (14, 7, 10, 5, 3)
BUF = tuple(8 * s + 2 * PAD for s in STRIPS)
SOLVES = (1, 2, 2, 2, 2)
UNROLL = (2, 7, 5, 5, 3)
DAMP = 0.8
NEAR = 8
F32 = jnp.float32


def loop(count, body, unroll=1):
    first, last = count if isinstance(count, tuple) else (0, count)
    if unroll >= last - first:
        for i in range(first, last):
            body(i)
    else:
        lax.fori_loop(first, last, lambda i, c: (body(i), c)[1], 0, unroll=unroll)


def at(i, offset, step=8):
    if isinstance(i, int):
        return pl.ds(i * step + offset, 8)
    return pl.ds(pl.multiple_of(i * step, step) + offset, 8)


def pairs_at(i, offset):
    base = i * 16 if isinstance(i, int) else pl.multiple_of(i * 16, 16)
    return pl.ds(base + offset, 8, stride=2), pl.ds(base + offset + 1, 8, stride=2)


def iota(dim):
    return lax.broadcasted_iota(jnp.int32, (8, LANES), dim)


def from_west(x):
    return jnp.where(iota(1) < 16, pltpu.roll(x, 17, 1), pltpu.roll(x, 16, 1))


def from_east(x):
    return jnp.where(iota(1) >= LANES - 16, pltpu.roll(x, LANES - 17, 1), pltpu.roll(x, LANES - 16, 1))


def side_values(x):
    return [from_west(x[-1])] + x[:-1], x[1:] + [from_east(x[0])]


def harmonic(a, b):
    return 2.0 * a * b / (a + b)


def make_weights(level, c_ref, a_ref, peers, strips=None, source_ref=None, b_ref=None):
    tiles = TILES[level]
    top, total_rows = first_row(level), peers * OWN[level]

    def body(i):
        c = [c_ref[t, at(i, PAD), :] for t in range(tiles)]
        row = top + i * 8 + iota(0)
        lane = iota(1)
        inside = jnp.logical_and(row >= 0, row < total_rows)
        west, east = side_values(c)
        west[0] = jnp.where(lane == 0, c[0], west[0])
        east[-1] = jnp.where(lane == LANES - 1, c[-1], east[-1])
        w_east = [harmonic(a, b) for a, b in zip(c, east)]
        w_west = [harmonic(c[0], west[0])] + w_east[:-1]
        for t in range(tiles):
            w_north = harmonic(c[t], jnp.where(row == 0, c[t], c_ref[t, at(i, PAD - 1), :]))
            w_south = harmonic(c[t], jnp.where(row == total_rows - 1, c[t], c_ref[t, at(i, PAD + 1), :]))
            diagonal = w_west[t] + w_east[t] + w_north + w_south
            gain = jnp.where(inside, DAMP / diagonal, 0.0)
            a_west, a_east = gain * w_west[t], gain * w_east[t]
            if t == 0:
                a_west = jnp.where(lane == 0, 0.0, a_west)
            if t == tiles - 1:
                a_east = jnp.where(lane == LANES - 1, 0.0, a_east)
            rows = at(i, 0)
            a_ref[0, t, rows, :] = a_west
            a_ref[1, t, rows, :] = a_east
            a_ref[2, t, rows, :] = gain * w_north
            a_ref[3, t, rows, :] = gain * w_south
            a_ref[4, t, rows, :] = gain
            a_ref[5, t, rows, :] = diagonal * (1.0 / DAMP)
            if source_ref is not None:
                b_ref[t, at(i, PAD), :] = gain * source_ref[t, at(i, PAD), :]

    loop(strips or STRIPS[level], body, UNROLL[level])


def sweep(level, v_ref, out_ref, b_ref, a_ref, finish, strips):
    tiles, solves = TILES[level], SOLVES[level]

    def body(i):
        v = [[v_ref[s * tiles + t, at(i, PAD), :] for t in range(tiles)] for s in range(solves)]
        sides = [side_values(x) for x in v]
        rows = at(i, 0)
        order = list(range(1, tiles - 1)) + ([0, tiles - 1] if tiles > 1 else [0])
        for t in order:
            a_west, a_east, a_north, a_south = (a_ref[k, t, rows, :] for k in range(4))
            for s in range(solves):
                west, east = sides[s]
                k = s * tiles + t
                north, south = v_ref[k, at(i, PAD - 1), :], v_ref[k, at(i, PAD + 1), :]
                moved = (a_north * north + a_south * south) + b_ref[k, at(i, PAD), :]
                moved += a_west * west[t] + a_east * east[t]
                out_ref[k, at(i, PAD), :] = finish(v[s][t], moved, t, rows)

    loop(strips or STRIPS[level], body, UNROLL[level])


def relax(level, v_ref, out_ref, b_ref, a_ref, strips=None):
    sweep(level, v_ref, out_ref, b_ref, a_ref, lambda v, moved, t, rows: (1.0 - DAMP) * v + moved, strips)


def residual(level, v_ref, out_ref, b_ref, a_ref, strips=None):
    def finish(v, moved, t, rows):
        return a_ref[5, t, rows, :] * (moved - DAMP * v)

    sweep(level, v_ref, out_ref, b_ref, a_ref, finish, strips)


def restrict(count, ref, offset, tiles, store, unroll=1):
    def body(j):
        even, odd = pairs_at(j, offset)
        for k in range(0, len(tiles), 2):
            a, b = tiles[k], tiles[k + 1]
            store(j, k // 2, (ref[a, even, :] + ref[a, odd, :]) + (ref[b, even, :] + ref[b, odd, :]))

    loop(count, body, unroll)


def prolong(count, e_ref, offset, e_tiles, v_ref, sign=1.0, v_offset=PAD, unroll=1):
    def body(j):
        halves = pairs_at(j, v_offset)
        for k, tile in enumerate(e_tiles):
            e = sign * e_ref[tile, at(j, offset), :]
            for t in (2 * k, 2 * k + 1):
                for rows in halves:
                    v_ref[t, rows, :] = v_ref[t, rows, :] + e

    loop(count, body, unroll)


def clear_pads(*refs, value=0.0, size=PAD):
    for ref in refs:
        tiles, rows, _ = ref.shape
        ref[:, 0:size, :] = jnp.full((tiles, size, LANES), value, F32)
        ref[:, rows - size : rows, :] = jnp.full((tiles, size, LANES), value, F32)


def fill(ref, value):
    def body(i):
        ref[:, at(i, 0), :] = jnp.full((ref.shape[0], 8, LANES), value, F32)

    loop(ref.shape[1] // 8, body)


def turn(groups):
    lane = iota(1)
    groups = [list(x) for x in groups]
    for step in (1, 2, 4, 8):
        upper = lax.rem(lane, 2 * step) >= step
        for i in range(16):
            if i & step == 0:
                j = i + step
                for x in groups:
                    from_j = pltpu.roll(x[j], step, 1)
                    from_i = pltpu.roll(x[i], LANES - step, 1)
                    x[i], x[j] = jnp.where(upper, from_j, x[i]), jnp.where(upper, x[j], from_i)
    return groups


def place():
    return lax.axis_index("grid")


def first_row(level):
    return place() * OWN[level] - HALO[level]


def towards_next():
    i = place()
    return lax.rem(i, 2) == 0, lax.rem(i, 4) < 2


def slab_positions():
    next_first, far = towards_next()
    return (
        jnp.where(next_first, 3, 1), jnp.where(next_first, 1, 3), jnp.where(far, 4, 0), jnp.where(far, 0, 4), 2,
    )


def convert(rows_of, log_ref, src_ref, c0, s0):
    tiles = TILES[0]
    for k in range(0, len(rows_of), 2):
        groups, places = [], []
        for row, to in rows_of[k : k + 2]:
            logs, sources = ([ref[row : row + 8, t * LANES : (t + 1) * LANES] for t in range(tiles)] for ref in (log_ref, src_ref))
            groups += [[jnp.exp(v) for v in logs], sources]
            places += [(c0, to), (s0, to)]
        for (ref, to), x in zip(places, turn(groups)):
            for t, v in enumerate(x):
                ref[t, to : to + 8, :] = v


def load(sems, *pairs):
    copies = [pltpu.make_async_copy(src, dst, sems.at[k]) for k, (src, dst) in enumerate(pairs)]
    for copy in copies:
        copy.start()
    return copies


def boundary_rows(near):
    count = NEAR if near else HALO[0] - NEAR
    start = 0 if near else NEAR
    return (start, count), (OWN[0] - start - count, count)


def write_messages(sides, c0, s0, first_ref, second_ref):
    tiles = TILES[0]
    next_first, _ = towards_next()
    up, down = (PAD + HALO[0] + start for start, _ in sides)
    for ref, base in ((first_ref, jnp.where(next_first, down, up)), (second_ref, jnp.where(next_first, up, down))):
        for i in range(sides[0][1] // 8):
            rows = pl.ds(pl.multiple_of(base + 8 * i, 8), 8)
            for t in range(tiles):
                ref[t, 8 * i : 8 * i + 8, :] = c0[t, rows, :]
                ref[tiles + t, 8 * i : 8 * i + 8, :] = s0[t, rows, :]


def pack_kernel(log_in, src_in, c0, s0, first_ref, second_ref, logs, sources, sems):
    sides = boundary_rows(True)
    parts = [pl.ds(start, count) for start, count in sides] + [pl.ds(NEAR, OWN[0] - 2 * NEAR)]
    copies = load(sems, *((ref.at[p, :], to.at[p, :]) for p in parts for ref, to in ((log_in, logs), (src_in, sources))))
    for copy in copies[:4]:
        copy.wait()
    convert([(start, PAD + HALO[0] + start) for start, _ in sides], logs, sources, c0, s0)
    write_messages(sides, c0, s0, first_ref, second_ref)
    for copy in copies[4:]:
        copy.wait()


def pack_rest_kernel(log_ref, src_ref, c0_in, s0_in, c0, s0, first_ref, second_ref):
    sides = boundary_rows(False)
    places = [start + k for start, count in sides for k in range(0, count, 8)]
    convert([(row, PAD + HALO[0] + row) for row in places], log_ref, src_ref, c0, s0)
    write_messages(sides, c0, s0, first_ref, second_ref)


def inner_kernel(peers, log_ref, src_ref, c0_in, s0_in, c0, s0, a0, bp0, va0, c1):
    halo, own, tiles = HALO[0], OWN[0], TILES[0]
    clear_pads(c0, value=1.0, size=PAD + halo)
    clear_pads(s0, bp0, va0, size=PAD + halo)
    clear_pads(c1, value=1.0)
    convert([(k, PAD + halo + k) for k in range(halo, own - halo, 8)], log_ref, src_ref, c0, s0)
    make_weights(0, c0, a0, peers, (4, 10), s0, bp0)
    restrict((2, 5), c0, PAD, range(tiles), quarter_store(c1))
    relax(0, bp0, va0, bp0, a0, (5, 9))


def insert(first_ref, second_ref, near, c0, s0):
    tiles = TILES[0]
    next_first, _ = towards_next()
    count = first_ref.shape[1]
    above = PAD + (HALO[0] - NEAR if near else 0)
    below = PAD + HALO[0] + OWN[0] + (0 if near else NEAR)
    for ref, base in ((first_ref, jnp.where(next_first, below, above)), (second_ref, jnp.where(next_first, above, below))):
        for i in range(count // 8):
            rows = pl.ds(pl.multiple_of(base + 8 * i, 8), 8)
            for t in range(tiles):
                c0[t, rows, :] = ref[t, 8 * i : 8 * i + 8, :]
                s0[t, rows, :] = ref[tiles + t, 8 * i : 8 * i + 8, :]


def scaled_store(bp_ref, a_ref, start=0):
    def store(j, k, q):
        bp_ref[start + k, at(j, PAD), :] = a_ref[4, k, at(j, 0), :] * q

    return store


def quarter_store(c_ref):
    def store(j, k, q):
        c_ref[k, at(j, PAD), :] = 0.25 * q

    return store


def outer_kernel(peers, *refs):
    first_ref, second_ref = refs[9:11]
    c0, s0, a0, bp0, va0, c1, a1, bp1, va1, vb0 = refs[11:]
    tiles = TILES[0]
    insert(first_ref, second_ref, False, c0, s0)
    clear_pads(vb0)
    ends = ((0, 2), (5, 7))
    for strips in ((0, 3), (11, 14)):
        make_weights(0, c0, a0, peers, strips, s0, bp0)
    for strips in ends:
        restrict(strips, c0, PAD, range(tiles), quarter_store(c1), 2)
    for strips in ends:
        make_weights(1, c1, a1, peers, strips)
        restrict(strips, s0, PAD, range(tiles), scaled_store(bp1, a1, TILES[1]), 2)
    for strips in ((0, 4), (10, 14)):
        relax(0, bp0, va0, bp0, a0, strips)
    for strips in ((0, 4), (10, 14)):
        residual(0, va0, vb0, bp0, a0, strips)
    for strips in ends:
        restrict(strips, vb0, PAD, range(tiles), scaled_store(bp1, a1), 2)
    relax(1, bp1, va1, bp1, a1)


def open_kernel(
    peers, c0_in, s0_in, a0_in, b0_in, v0_in, c1_in, first_ref, second_ref,
    c0, s0, a0, bp0, va0, c1, a1, bp1, va1, msg_ref,
    vb0, vb1,
):
    tiles = TILES[0]
    insert(first_ref, second_ref, True, c0, s0)
    clear_pads(va1, vb1, size=2 * PAD)
    clear_pads(bp1, size=2 * PAD)
    for strips in ((2, 4), (10, 12)):
        make_weights(0, c0, a0, peers, strips, s0, bp0)
    for strips in ((1, 2), (5, 6)):
        restrict(strips, c0, PAD, range(tiles), quarter_store(c1), 2)
    make_weights(1, c1, a1, peers, (1, 6))
    restrict((1, 6), s0, PAD, range(tiles), scaled_store(bp1, a1, TILES[1]))
    for strips in ((2, 5), (9, 12)):
        relax(0, bp0, va0, bp0, a0, strips)
    residual(0, va0, vb0, bp0, a0, (2, 12))
    restrict((1, 6), vb0, PAD, range(tiles), scaled_store(bp1, a1))
    relax(1, bp1, va1, bp1, a1, (1, 6))
    residual(1, va1, vb1, bp1, a1, (1, 6))

    def store(j, k, q):
        msg_ref[k, at(j, 0), :] = q

    restrict(OWN[2] // 8, vb1, PAD + HALO[1], range(2 * TILES[1]), store, 2)

    def store_coef(j, k, q):
        msg_ref[2 * TILES[2] + k, at(j, 0), :] = 0.25 * q

    restrict(OWN[2] // 8, c1, PAD + HALO[1], range(TILES[1]), store_coef, 2)


def deep_solve(a, bp, va, vb):
    relax(2, bp[2], va[2], bp[2], a[2])
    residual(2, va[2], vb[2], bp[2], a[2])
    for s in range(2):
        restrict(STRIPS[3], vb[2], PAD, range(s * 4, s * 4 + 4), scaled_store(bp[3], a[3], s * 2), 5)
    relax(3, bp[3], va[3], bp[3], a[3])
    residual(3, va[3], vb[3], bp[3], a[3])
    for s in range(2):
        restrict(STRIPS[4], vb[3], PAD, range(s * 2, s * 2 + 2), scaled_store(bp[4], a[4], s), 3)
    relax(4, bp[4], va[4], bp[4], a[4])
    relax(4, va[4], vb[4], bp[4], a[4])
    relax(4, vb[4], va[4], bp[4], a[4])
    prolong(2, va[4], PAD, range(2), va[3], unroll=2)
    relax(3, va[3], vb[3], bp[3], a[3], (0, 5))
    relax(3, vb[3], va[3], bp[3], a[3], (1, 4))
    prolong((1, 4), va[3], PAD, range(4), va[2], unroll=3)
    relax(2, va[2], vb[2], bp[2], a[2], (3, 7))
    relax(2, vb[2], va[2], bp[2], a[2], (3, 7))


def up_level_1(va2, va1, vb1, bp1, a1, strips=(0, 7)):
    offset = PAD + HALO[2] - HALO[1] // 2
    prolong(4, va2, offset, range(2 * TILES[2]), va1)
    relax(1, va1, vb1, bp1, a1, strips)
    relax(1, vb1, va1, bp1, a1, strips)


def up_level_0(va1, va0, vb0, bp0, a0, first, second):
    prolong(STRIPS[1], va1, PAD, range(TILES[1]), va0)
    relax(0, va0, vb0, bp0, a0, first)
    relax(0, vb0, va0, bp0, a0, second)


def assemble(messages, a2, bp2):
    for position, m in zip(slab_positions(), messages):
        for i in range(2):
            row = pl.multiple_of(position * OWN[2] + i * 8, 8)
            for k in range(2 * TILES[2]):
                bp2[k, pl.ds(PAD + row, 8), :] = (
                    a2[4, k % TILES[2], pl.ds(row, 8), :] * m[k, i * 8 : i * 8 + 8, :]
                )


def middle_kernel(
    peers, m0, m1, m2, m3, m4, a0, bp0, va0_in, a1, bp1_in, va1_in,
    msg_ref, a2, a3, a4, va0, bp1, va1,
    vb0, vb1, c2, bp2, va2, vb2, c3, bp3, va3, vb3, c4, bp4, va4, vb4,
):
    messages = (m0, m1, m2, m3, m4)
    fill(c4, 1.0)
    clear_pads(c2, c3, value=1.0)
    for ref in (bp4, va4, vb4):
        fill(ref, 0.0)
    clear_pads(bp2, va2, vb2, bp3, va3, vb3)
    clear_pads(vb0, vb1, size=2 * PAD)
    for position, m in zip(slab_positions(), messages):
        for i in range(2):
            row = pl.multiple_of(position * OWN[2] + i * 8, 8)
            for k in range(TILES[2]):
                c2[k, pl.ds(PAD + row, 8), :] = m[2 * TILES[2] + k, i * 8 : i * 8 + 8, :]
    make_weights(2, c2, a2, peers)
    restrict(STRIPS[3], c2, PAD, range(4), quarter_store(c3), 5)
    make_weights(3, c3, a3, peers)
    restrict(2, c3, PAD, range(2), quarter_store(c4), 2)

    def last_rows(j, k, q):
        c4[k, PAD + 16 : PAD + 24, :] = jnp.where(iota(0) < ROWS[4] - 16, 0.25 * q, 1.0)

    restrict(1, c3, PAD + 32, range(2), last_rows)
    make_weights(4, c4, a4, peers)
    assemble(messages, a2, bp2)
    a = {2: a2, 3: a3, 4: a4}
    bp = {2: bp2, 3: bp3, 4: bp4}
    va = {2: va2, 3: va3, 4: va4}
    vb = {2: vb2, 3: vb3, 4: vb4}
    deep_solve(a, bp, va, vb)
    up_level_1(va2, va1, vb1, bp1, a1)
    up_level_0(va1, va0, vb0, bp0, a0, (1, 13), (1, 13))

    relax(0, va0, vb0, bp0, a0, (1, 13))
    relax(0, vb0, va0, bp0, a0, (1, 13))
    residual(0, va0, vb0, bp0, a0, (1, 13))
    restrict((1, 6), vb0, PAD, range(TILES[0]), scaled_store(bp1, a1))

    def clear(i):
        va1[0 : TILES[1], at(i, 0), :] = jnp.zeros((TILES[1], 8, LANES), F32)

    loop(BUF[1] // 8, clear)
    relax(1, va1, vb1, bp1, a1)
    relax(1, vb1, va1, bp1, a1)
    residual(1, va1, vb1, bp1, a1, (1, 6))

    def store(j, k, q):
        msg_ref[k, at(j, 0), :] = q

    restrict(OWN[2] // 8, vb1, PAD + HALO[1], range(2 * TILES[1]), store, 2)


def close_kernel(
    m0, m1, m2, m3, m4, a0, bp0, va0_in, a1, bp1, va1_in, a2, a3, a4,
    va0, va1, out_hbm, mine_ref, other_ref,
    vb0, vb1, bp2, va2, vb2, bp3, va3, vb3, bp4, va4, vb4, out_ref, sems,
):
    for ref in (bp4, va4, vb4):
        fill(ref, 0.0)
    clear_pads(bp2, va2, vb2, bp3, va3, vb3)
    clear_pads(vb0, vb1, size=2 * PAD)
    assemble((m0, m1, m2, m3, m4), a2, bp2)
    a = {2: a2, 3: a3, 4: a4}
    bp = {2: bp2, 3: bp3, 4: bp4}
    va = {2: va2, 3: va3, 4: va4}
    vb = {2: vb2, 3: vb3, 4: vb4}
    deep_solve(a, bp, va, vb)
    up_level_1(va2, va1, vb1, bp1, a1, (1, 6))
    up_level_0(va1, va0, vb0, bp0, a0, (2, 12), (3, 11))
    prolong(OWN[1] // 8, va1, PAD + HALO[1], range(TILES[1], 2 * TILES[1]), va0, -1.0, PAD + HALO[0])
    tiles = TILES[0]
    left = lax.axis_index("samp") == 0

    copies = []
    for piece in range(OWN[0] // 16):
        strips = (2 * piece, 2 * piece + 1)
        turned = turn([[va0[t, at(j, PAD + HALO[0]), :] for t in range(tiles)] for j in strips])
        for j, x in zip(strips, turned):
            for t in range(tiles):
                out_ref[at(j, 0), t * LANES : (t + 1) * LANES] = x[t]
            for t in range(tiles // 2):
                low, high = x[t], x[tiles // 2 + t]
                mine_ref[at(j, 0), t * LANES : (t + 1) * LANES] = jnp.where(left, low, high)
                other_ref[at(j, 0), t * LANES : (t + 1) * LANES] = jnp.where(left, high, low)
        rows = pl.ds(16 * piece, 16)
        copies.append(pltpu.make_async_copy(out_ref.at[rows, :], out_hbm.at[rows, :], sems.at[piece]))
        copies[-1].start()
    for copy in copies:
        copy.wait()


VMEM = pl.BlockSpec(memory_space=pltpu.VMEM)


def near(*dims):
    return pltpu.VMEM(dims, F32)


def held(*values):
    return [pltpu.with_memory_space_constraint(v, pltpu.VMEM) for v in values]


def a_shape(level):
    return (6, TILES[level], 8 * STRIPS[level], LANES)


def v_shape(level):
    return (SOLVES[level] * TILES[level], BUF[level], LANES)


def c_shape(level):
    return (TILES[level], BUF[level], LANES)


FAR = pl.BlockSpec(memory_space=pltpu.HBM)


def call(kernel, arguments, outputs, scratch=(), aliases=None, sems=0, far=0):
    return pl.pallas_call(
        kernel,
        out_shape=outputs,
        in_specs=[FAR] * far + [VMEM] * (len(arguments) - far),
        out_specs=[FAR if isinstance(o, jax.ShapeDtypeStruct) else VMEM for o in outputs],
        scratch_shapes=[pltpu.VMEM(s, F32) for s in scratch] + ([pltpu.SemaphoreType.DMA((sems,))] if sems else []),
        input_output_aliases=aliases or {},
        compiler_params=pltpu.CompilerParams(vmem_limit_bytes=24 * 2**20),
        cost_estimate=pl.CostEstimate(flops=10**8, bytes_accessed=10**6, transcendentals=0),
    )(*arguments)


def swaps(distance):
    peers, samples = lax.axis_size("grid"), lax.axis_size("samp")
    even = [(i, i + distance if i % (2 * distance) < distance else i - distance) for i in range(peers)]
    odd = [(a + distance, b + distance) for a, b in even if max(a, b) + distance < peers]
    ends = sorted(set(range(peers)) - {a for a, _ in odd})
    both = [[(s * peers + a, s * peers + b) for s in range(samples) for a, b in pairs] for pairs in (even, odd)]
    both[1] += [(s * peers + e, (s + 1) % samples * peers + e) for s in range(samples) for e in ends]
    return both


def swapped(value, pairs):
    return lax.ppermute(value, ("samp", "grid"), pairs)


def gathered(value):
    sets = [pairs for distance in (1, 2) for pairs in swaps(distance)]
    return [swapped(value, pairs) for pairs in sets] + [value]


def local(log_coef, source):
    peers = lax.axis_size("grid")
    log_field, source_field = log_coef[0], source[0]
    rows, columns = source_field.shape
    far_fields = [pltpu.with_memory_space_constraint(x, pltpu.HBM) for x in (log_field, source_field)]
    tiled = [near(*c_shape(0)), near(*c_shape(0))]
    even, odd = swaps(1)
    edge = near(2 * TILES[0], NEAR, LANES)
    c0, s0, first, second, *fields = call(
        pack_kernel, far_fields, tiled + [edge, edge] + [near(rows, columns)] * 2, sems=6, far=2
    )
    near_rows = [swapped(first, even), swapped(second, odd)]
    edge = near(2 * TILES[0], HALO[0] - NEAR, LANES)
    c0, s0, first, second = call(pack_rest_kernel, held(*fields, c0, s0), tiled + [edge, edge], aliases={2: 0, 3: 1})
    rest_rows = [swapped(first, even), swapped(second, odd)]
    state = [near(*f(level)) for level in (0, 1) for f in (a_shape, v_shape, v_shape)]
    whole = tiled + state[:3] + [near(*c_shape(1))]
    started = call(functools.partial(inner_kernel, peers), held(*fields, c0, s0), whole, aliases={2: 0, 3: 1})
    *opened, message = call(
        functools.partial(open_kernel, peers), held(*started, *near_rows),
        whole + state[3:] + [near(3 * TILES[2], OWN[2], LANES)],
        [v_shape(0), v_shape(1)], {k: k for k in range(6)},
    )
    arrived = gathered(message)
    c0, s0, a0, b0, v0, _, a1, b1, v1 = call(
        functools.partial(outer_kernel, peers), held(*opened, *rest_rows),
        whole + state[3:], [v_shape(0)], {k: k for k in range(9)},
    )
    deep = [shape for level in (2, 3, 4) for shape in [c_shape(level)] + [v_shape(level)] * 3]
    message, a2, a3, a4, v0, b1, v1 = call(
        functools.partial(middle_kernel, peers),
        held(*arrived, a0, b0, v0, a1, b1, v1),
        [near(2 * TILES[2], OWN[2], LANES)] + [near(*a_shape(level)) for level in (2, 3, 4)] + [state[k] for k in (2, 4, 5)],
        [v_shape(0), v_shape(1)] + deep,
        {7: 4, 9: 5, 10: 6},
    )
    deep = [shape for level in (2, 3, 4) for shape in [v_shape(level)] * 3]
    half = near(rows, columns // 2)
    v0, v1, correction, mine, other = call(
        close_kernel,
        held(*gathered(message), a0, b0, v0, a1, b1, v1, a2, a3, a4),
        (state[2], state[5], jax.ShapeDtypeStruct((rows, columns), F32), half, half),
        [v_shape(0), v_shape(1)] + deep + [(rows, columns)],
        {7: 0, 10: 1},
        sems=rows // 16,
    )

    theirs = lax.ppermute(other, "samp", [(0, 1), (1, 0)])
    samples = lax.axis_size("samp")
    level_mean = (mine + theirs) / samples
    squares = mine * mine + theirs * theirs
    level_var = (squares - samples * level_mean * level_mean) / (samples - 1)
    return (correction[None], level_mean, level_var)


def solution(mesh):
    in_specs = (P("samp", "grid", None), P("samp", "grid", None))
    out_specs = (P("samp", "grid", None), P("grid", "samp"), P("grid", "samp"))
    return jax.shard_map(local, mesh=mesh, in_specs=in_specs, out_specs=out_specs, check_vma=False)
```

```python
import functools

import jax
import jax.numpy as jnp
from jax import lax
from jax.experimental import pallas as pl
from jax.experimental.pallas import tpu as pltpu
from jax.sharding import PartitionSpec as P


LANES = 128
PAD = 8
OWN = (64, 32, 16, 8, 4)
HALO = (24, 12, 32, 16, 8)
ROWS = tuple(o + 2 * h for o, h in zip(OWN, HALO))
TILES = (16, 8, 4, 2, 1)
STRIPS = (14, 7, 10, 5, 3)
BUF = tuple(8 * s + 2 * PAD for s in STRIPS)
SOLVES = (1, 2, 2, 2, 2)
UNROLL = (2, 7, 5, 5, 3)
DAMP = 0.8
NEAR = 8
F32 = jnp.float32


def loop(count, body, unroll=1):
    first, last = count if isinstance(count, tuple) else (0, count)
    if unroll >= last - first:
        for i in range(first, last):
            body(i)
    else:
        lax.fori_loop(first, last, lambda i, c: (body(i), c)[1], 0, unroll=unroll)


def at(i, offset, step=8):
    if isinstance(i, int):
        return pl.ds(i * step + offset, 8)
    return pl.ds(pl.multiple_of(i * step, step) + offset, 8)


def pairs_at(i, offset):
    base = i * 16 if isinstance(i, int) else pl.multiple_of(i * 16, 16)
    return pl.ds(base + offset, 8, stride=2), pl.ds(base + offset + 1, 8, stride=2)


def iota(dim):
    return lax.broadcasted_iota(jnp.int32, (8, LANES), dim)


def from_west(x):
    return jnp.where(iota(1) < 16, pltpu.roll(x, 17, 1), pltpu.roll(x, 16, 1))


def from_east(x):
    return jnp.where(iota(1) >= LANES - 16, pltpu.roll(x, LANES - 17, 1), pltpu.roll(x, LANES - 16, 1))


def side_values(x):
    return [from_west(x[-1])] + x[:-1], x[1:] + [from_east(x[0])]


def harmonic(a, b):
    return 2.0 * a * b / (a + b)


def make_weights(level, c_ref, a_ref, peers, strips=None, source_ref=None, b_ref=None):
    tiles = TILES[level]
    top, total_rows = first_row(level), peers * OWN[level]

    def body(i):
        c = [c_ref[t, at(i, PAD), :] for t in range(tiles)]
        row = top + i * 8 + iota(0)
        lane = iota(1)
        inside = jnp.logical_and(row >= 0, row < total_rows)
        west, east = side_values(c)
        west[0] = jnp.where(lane == 0, c[0], west[0])
        east[-1] = jnp.where(lane == LANES - 1, c[-1], east[-1])
        w_east = [harmonic(a, b) for a, b in zip(c, east)]
        w_west = [harmonic(c[0], west[0])] + w_east[:-1]
        for t in range(tiles):
            w_north = harmonic(c[t], jnp.where(row == 0, c[t], c_ref[t, at(i, PAD - 1), :]))
            w_south = harmonic(c[t], jnp.where(row == total_rows - 1, c[t], c_ref[t, at(i, PAD + 1), :]))
            diagonal = w_west[t] + w_east[t] + w_north + w_south
            gain = jnp.where(inside, DAMP / diagonal, 0.0)
            a_west, a_east = gain * w_west[t], gain * w_east[t]
            if t == 0:
                a_west = jnp.where(lane == 0, 0.0, a_west)
            if t == tiles - 1:
                a_east = jnp.where(lane == LANES - 1, 0.0, a_east)
            rows = at(i, 0)
            a_ref[0, t, rows, :] = a_west
            a_ref[1, t, rows, :] = a_east
            a_ref[2, t, rows, :] = gain * w_north
            a_ref[3, t, rows, :] = gain * w_south
            a_ref[4, t, rows, :] = gain
            a_ref[5, t, rows, :] = diagonal * (1.0 / DAMP)
            if source_ref is not None:
                b_ref[t, at(i, PAD), :] = gain * source_ref[t, at(i, PAD), :]

    loop(strips or STRIPS[level], body, UNROLL[level])


def sweep(level, v_ref, out_ref, b_ref, a_ref, finish, strips):
    tiles, solves = TILES[level], SOLVES[level]

    def body(i):
        v = [[v_ref[s * tiles + t, at(i, PAD), :] for t in range(tiles)] for s in range(solves)]
        sides = [side_values(x) for x in v]
        rows = at(i, 0)
        order = list(range(1, tiles - 1)) + ([0, tiles - 1] if tiles > 1 else [0])
        for t in order:
            a_west, a_east, a_north, a_south = (a_ref[k, t, rows, :] for k in range(4))
            for s in range(solves):
                west, east = sides[s]
                k = s * tiles + t
                north, south = v_ref[k, at(i, PAD - 1), :], v_ref[k, at(i, PAD + 1), :]
                moved = (a_north * north + a_south * south) + b_ref[k, at(i, PAD), :]
                moved += a_west * west[t] + a_east * east[t]
                out_ref[k, at(i, PAD), :] = finish(v[s][t], moved, t, rows)

    loop(strips or STRIPS[level], body, UNROLL[level])


def relax(level, v_ref, out_ref, b_ref, a_ref, strips=None):
    sweep(level, v_ref, out_ref, b_ref, a_ref, lambda v, moved, t, rows: (1.0 - DAMP) * v + moved, strips)


def residual(level, v_ref, out_ref, b_ref, a_ref, strips=None):
    def finish(v, moved, t, rows):
        return a_ref[5, t, rows, :] * (moved - DAMP * v)

    sweep(level, v_ref, out_ref, b_ref, a_ref, finish, strips)


def restrict(count, ref, offset, tiles, store, unroll=1):
    def body(j):
        even, odd = pairs_at(j, offset)
        for k in range(0, len(tiles), 2):
            a, b = tiles[k], tiles[k + 1]
            store(j, k // 2, (ref[a, even, :] + ref[a, odd, :]) + (ref[b, even, :] + ref[b, odd, :]))

    loop(count, body, unroll)


def prolong(count, e_ref, offset, e_tiles, v_ref, sign=1.0, v_offset=PAD, unroll=1):
    def body(j):
        halves = pairs_at(j, v_offset)
        for k, tile in enumerate(e_tiles):
            e = sign * e_ref[tile, at(j, offset), :]
            for t in (2 * k, 2 * k + 1):
                for rows in halves:
                    v_ref[t, rows, :] = v_ref[t, rows, :] + e

    loop(count, body, unroll)


def clear_pads(*refs, value=0.0, size=PAD):
    for ref in refs:
        tiles, rows, _ = ref.shape
        ref[:, 0:size, :] = jnp.full((tiles, size, LANES), value, F32)
        ref[:, rows - size : rows, :] = jnp.full((tiles, size, LANES), value, F32)


def fill(ref, value):
    def body(i):
        ref[:, at(i, 0), :] = jnp.full((ref.shape[0], 8, LANES), value, F32)

    loop(ref.shape[1] // 8, body)


def turn(groups):
    lane = iota(1)
    groups = [list(x) for x in groups]
    for step in (1, 2, 4, 8):
        upper = lax.rem(lane, 2 * step) >= step
        for i in range(16):
            if i & step == 0:
                j = i + step
                for x in groups:
                    from_j = pltpu.roll(x[j], step, 1)
                    from_i = pltpu.roll(x[i], LANES - step, 1)
                    x[i], x[j] = jnp.where(upper, from_j, x[i]), jnp.where(upper, x[j], from_i)
    return groups


def place():
    return lax.axis_index("grid")


def first_row(level):
    return place() * OWN[level] - HALO[level]


def towards_next():
    i = place()
    return lax.rem(i, 2) == 0, lax.rem(i, 4) < 2


def slab_positions():
    next_first, far = towards_next()
    return (
        jnp.where(next_first, 3, 1), jnp.where(next_first, 1, 3), jnp.where(far, 4, 0), jnp.where(far, 0, 4), 2,
    )


def convert(rows_of, log_ref, src_ref, c0, s0):
    tiles = TILES[0]
    for k in range(0, len(rows_of), 2):
        groups, places = [], []
        for row, to in rows_of[k : k + 2]:
            logs, sources = ([ref[row : row + 8, t * LANES : (t + 1) * LANES] for t in range(tiles)] for ref in (log_ref, src_ref))
            groups += [[jnp.exp(v) for v in logs], sources]
            places += [(c0, to), (s0, to)]
        for (ref, to), x in zip(places, turn(groups)):
            for t, v in enumerate(x):
                ref[t, to : to + 8, :] = v


def load(sems, *pairs):
    copies = [pltpu.make_async_copy(src, dst, sems.at[k]) for k, (src, dst) in enumerate(pairs)]
    for copy in copies:
        copy.start()
    return copies


def boundary_rows(near):
    count = NEAR if near else HALO[0] - NEAR
    start = 0 if near else NEAR
    return (start, count), (OWN[0] - start - count, count)


def write_messages(sides, c0, s0, first_ref, second_ref):
    tiles = TILES[0]
    next_first, _ = towards_next()
    up, down = (PAD + HALO[0] + start for start, _ in sides)
    for ref, base in ((first_ref, jnp.where(next_first, down, up)), (second_ref, jnp.where(next_first, up, down))):
        for i in range(sides[0][1] // 8):
            rows = pl.ds(pl.multiple_of(base + 8 * i, 8), 8)
            for t in range(tiles):
                ref[t, 8 * i : 8 * i + 8, :] = c0[t, rows, :]
                ref[tiles + t, 8 * i : 8 * i + 8, :] = s0[t, rows, :]


def pack_kernel(log_in, src_in, c0, s0, first_ref, second_ref, logs, sources, sems):
    sides = boundary_rows(True)
    parts = [pl.ds(start, count) for start, count in sides] + [pl.ds(NEAR, OWN[0] - 2 * NEAR)]
    copies = load(sems, *((ref.at[p, :], to.at[p, :]) for p in parts for ref, to in ((log_in, logs), (src_in, sources))))
    for copy in copies[:4]:
        copy.wait()
    convert([(start, PAD + HALO[0] + start) for start, _ in sides], logs, sources, c0, s0)
    write_messages(sides, c0, s0, first_ref, second_ref)
    for copy in copies[4:]:
        copy.wait()


def pack_rest_kernel(log_ref, src_ref, c0_in, s0_in, c0, s0, first_ref, second_ref):
    sides = boundary_rows(False)
    places = [start + k for start, count in sides for k in range(0, count, 8)]
    convert([(row, PAD + HALO[0] + row) for row in places], log_ref, src_ref, c0, s0)
    write_messages(sides, c0, s0, first_ref, second_ref)


def inner_kernel(peers, log_ref, src_ref, c0_in, s0_in, c0, s0, a0, bp0, va0, c1):
    halo, own, tiles = HALO[0], OWN[0], TILES[0]
    clear_pads(c0, value=1.0, size=PAD + halo)
    clear_pads(s0, bp0, va0, size=PAD + halo)
    clear_pads(c1, value=1.0)
    convert([(k, PAD + halo + k) for k in range(halo, own - halo, 8)], log_ref, src_ref, c0, s0)
    make_weights(0, c0, a0, peers, (4, 10), s0, bp0)
    restrict((2, 5), c0, PAD, range(tiles), quarter_store(c1))
    relax(0, bp0, va0, bp0, a0, (5, 9))


def insert(first_ref, second_ref, near, c0, s0):
    tiles = TILES[0]
    next_first, _ = towards_next()
    count = first_ref.shape[1]
    above = PAD + (HALO[0] - NEAR if near else 0)
    below = PAD + HALO[0] + OWN[0] + (0 if near else NEAR)
    for ref, base in ((first_ref, jnp.where(next_first, below, above)), (second_ref, jnp.where(next_first, above, below))):
        for i in range(count // 8):
            rows = pl.ds(pl.multiple_of(base + 8 * i, 8), 8)
            for t in range(tiles):
                c0[t, rows, :] = ref[t, 8 * i : 8 * i + 8, :]
                s0[t, rows, :] = ref[tiles + t, 8 * i : 8 * i + 8, :]


def scaled_store(bp_ref, a_ref, start=0):
    def store(j, k, q):
        bp_ref[start + k, at(j, PAD), :] = a_ref[4, k, at(j, 0), :] * q

    return store


def quarter_store(c_ref):
    def store(j, k, q):
        c_ref[k, at(j, PAD), :] = 0.25 * q

    return store


def outer_kernel(peers, *refs):
    first_ref, second_ref = refs[9:11]
    c0, s0, a0, bp0, va0, c1, a1, bp1, va1, vb0 = refs[11:]
    tiles = TILES[0]
    insert(first_ref, second_ref, False, c0, s0)
    clear_pads(vb0)
    ends = ((0, 2), (5, 7))
    for strips in ((0, 3), (11, 14)):
        make_weights(0, c0, a0, peers, strips, s0, bp0)
    for strips in ends:
        restrict(strips, c0, PAD, range(tiles), quarter_store(c1), 2)
    for strips in ends:
        make_weights(1, c1, a1, peers, strips)
        restrict(strips, s0, PAD, range(tiles), scaled_store(bp1, a1, TILES[1]), 2)
    for strips in ((0, 4), (10, 14)):
        relax(0, bp0, va0, bp0, a0, strips)
    for strips in ((0, 4), (10, 14)):
        residual(0, va0, vb0, bp0, a0, strips)
    for strips in ends:
        restrict(strips, vb0, PAD, range(tiles), scaled_store(bp1, a1), 2)
    relax(1, bp1, va1, bp1, a1)


def open_kernel(
    peers, c0_in, s0_in, a0_in, b0_in, v0_in, c1_in, first_ref, second_ref,
    c0, s0, a0, bp0, va0, c1, a1, bp1, va1, msg_ref,
    vb0, vb1,
):
    tiles = TILES[0]
    insert(first_ref, second_ref, True, c0, s0)
    clear_pads(va1, vb1, size=2 * PAD)
    clear_pads(bp1, size=2 * PAD)
    for strips in ((2, 4), (10, 12)):
        make_weights(0, c0, a0, peers, strips, s0, bp0)
    for strips in ((1, 2), (5, 6)):
        restrict(strips, c0, PAD, range(tiles), quarter_store(c1), 2)
    make_weights(1, c1, a1, peers, (1, 6))
    restrict((1, 6), s0, PAD, range(tiles), scaled_store(bp1, a1, TILES[1]))
    for strips in ((2, 5), (9, 12)):
        relax(0, bp0, va0, bp0, a0, strips)
    residual(0, va0, vb0, bp0, a0, (2, 12))
    restrict((1, 6), vb0, PAD, range(tiles), scaled_store(bp1, a1))
    relax(1, bp1, va1, bp1, a1, (1, 6))
    residual(1, va1, vb1, bp1, a1, (1, 6))

    def store(j, k, q):
        msg_ref[k, at(j, 0), :] = q

    restrict(OWN[2] // 8, vb1, PAD + HALO[1], range(2 * TILES[1]), store, 2)

    def store_coef(j, k, q):
        msg_ref[2 * TILES[2] + k, at(j, 0), :] = 0.25 * q

    restrict(OWN[2] // 8, c1, PAD + HALO[1], range(TILES[1]), store_coef, 2)


def deep_solve(a, bp, va, vb):
    relax(2, bp[2], va[2], bp[2], a[2])
    residual(2, va[2], vb[2], bp[2], a[2])
    for s in range(2):
        restrict(STRIPS[3], vb[2], PAD, range(s * 4, s * 4 + 4), scaled_store(bp[3], a[3], s * 2), 5)
    relax(3, bp[3], va[3], bp[3], a[3])
    residual(3, va[3], vb[3], bp[3], a[3])
    for s in range(2):
        restrict(STRIPS[4], vb[3], PAD, range(s * 2, s * 2 + 2), scaled_store(bp[4], a[4], s), 3)
    relax(4, bp[4], va[4], bp[4], a[4])
    relax(4, va[4], vb[4], bp[4], a[4])
    relax(4, vb[4], va[4], bp[4], a[4])
    prolong(2, va[4], PAD, range(2), va[3], unroll=2)
    relax(3, va[3], vb[3], bp[3], a[3], (0, 5))
    relax(3, vb[3], va[3], bp[3], a[3], (1, 4))
    prolong((1, 4), va[3], PAD, range(4), va[2], unroll=3)
    relax(2, va[2], vb[2], bp[2], a[2], (3, 7))
    relax(2, vb[2], va[2], bp[2], a[2], (3, 7))


def up_level_1(va2, va1, vb1, bp1, a1, strips=(0, 7)):
    offset = PAD + HALO[2] - HALO[1] // 2
    prolong(4, va2, offset, range(2 * TILES[2]), va1)
    relax(1, va1, vb1, bp1, a1, strips)
    relax(1, vb1, va1, bp1, a1, strips)


def up_level_0(va1, va0, vb0, bp0, a0, first, second, coarse=STRIPS[1]):
    prolong(coarse, va1, PAD, range(TILES[1]), va0)
    relax(0, va0, vb0, bp0, a0, first)
    relax(0, vb0, va0, bp0, a0, second)


def assemble(messages, a2, bp2):
    for position, m in zip(slab_positions(), messages):
        for i in range(2):
            row = pl.multiple_of(position * OWN[2] + i * 8, 8)
            for k in range(2 * TILES[2]):
                bp2[k, pl.ds(PAD + row, 8), :] = (
                    a2[4, k % TILES[2], pl.ds(row, 8), :] * m[k, i * 8 : i * 8 + 8, :]
                )


def middle_kernel(
    peers, m0, m1, m2, m3, m4, a0, bp0, va0_in, a1, bp1_in, va1_in,
    msg_ref, a2, a3, a4, va0, bp1, va1,
    vb0, vb1, c2, bp2, va2, vb2, c3, bp3, va3, vb3, c4, bp4, va4, vb4,
):
    messages = (m0, m1, m2, m3, m4)
    fill(c4, 1.0)
    clear_pads(c2, c3, value=1.0)
    for ref in (bp4, va4, vb4):
        fill(ref, 0.0)
    clear_pads(bp2, va2, vb2, bp3, va3, vb3)
    clear_pads(vb0, vb1, size=2 * PAD)
    for position, m in zip(slab_positions(), messages):
        for i in range(2):
            row = pl.multiple_of(position * OWN[2] + i * 8, 8)
            for k in range(TILES[2]):
                c2[k, pl.ds(PAD + row, 8), :] = m[2 * TILES[2] + k, i * 8 : i * 8 + 8, :]
    make_weights(2, c2, a2, peers)
    restrict(STRIPS[3], c2, PAD, range(4), quarter_store(c3), 5)
    make_weights(3, c3, a3, peers)
    restrict(2, c3, PAD, range(2), quarter_store(c4), 2)

    def last_rows(j, k, q):
        c4[k, PAD + 16 : PAD + 24, :] = jnp.where(iota(0) < ROWS[4] - 16, 0.25 * q, 1.0)

    restrict(1, c3, PAD + 32, range(2), last_rows)
    make_weights(4, c4, a4, peers)
    assemble(messages, a2, bp2)
    a = {2: a2, 3: a3, 4: a4}
    bp = {2: bp2, 3: bp3, 4: bp4}
    va = {2: va2, 3: va3, 4: va4}
    vb = {2: vb2, 3: vb3, 4: vb4}
    deep_solve(a, bp, va, vb)
    up_level_1(va2, va1, vb1, bp1, a1)
    up_level_0(va1, va0, vb0, bp0, a0, (1, 13), (1, 13))

    relax(0, va0, vb0, bp0, a0, (1, 13))
    relax(0, vb0, va0, bp0, a0, (1, 13))
    residual(0, va0, vb0, bp0, a0, (2, 12))
    restrict((1, 6), vb0, PAD, range(TILES[0]), scaled_store(bp1, a1))

    def clear(i):
        va1[0 : TILES[1], at(i, 0), :] = jnp.zeros((TILES[1], 8, LANES), F32)

    loop(BUF[1] // 8, clear)
    relax(1, va1, vb1, bp1, a1)
    relax(1, vb1, va1, bp1, a1)
    residual(1, va1, vb1, bp1, a1, (1, 6))

    def store(j, k, q):
        msg_ref[k, at(j, 0), :] = q

    restrict(OWN[2] // 8, vb1, PAD + HALO[1], range(2 * TILES[1]), store, 2)


def close_kernel(
    m0, m1, m2, m3, m4, a0, bp0, va0_in, a1, bp1, va1_in, a2, a3, a4,
    va0, va1, out_ref, mine_ref, other_ref,
    vb0, vb1, bp2, va2, vb2, bp3, va3, vb3, bp4, va4, vb4,
):
    for ref in (bp4, va4, vb4):
        fill(ref, 0.0)
    clear_pads(bp2, va2, vb2, bp3, va3, vb3)
    clear_pads(vb0, vb1, size=2 * PAD)
    assemble((m0, m1, m2, m3, m4), a2, bp2)
    a = {2: a2, 3: a3, 4: a4}
    bp = {2: bp2, 3: bp3, 4: bp4}
    va = {2: va2, 3: va3, 4: va4}
    vb = {2: vb2, 3: vb3, 4: vb4}
    deep_solve(a, bp, va, vb)
    up_level_1(va2, va1, vb1, bp1, a1, (1, 6))
    up_level_0(va1, va0, vb0, bp0, a0, (2, 12), (3, 11), (1, 6))
    prolong(OWN[1] // 8, va1, PAD + HALO[1], range(TILES[1], 2 * TILES[1]), va0, -1.0, PAD + HALO[0])
    tiles = TILES[0]
    left = lax.axis_index("samp") == 0

    for piece in range(0, OWN[0] // 8, 4):
        strips = range(piece, piece + 4)
        turned = turn([[va0[t, at(j, PAD + HALO[0]), :] for t in range(tiles)] for j in strips])
        for j, x in zip(strips, turned):
            for t in range(tiles):
                out_ref[at(j, 0), t * LANES : (t + 1) * LANES] = x[t]
            for t in range(tiles // 2):
                low, high = x[t], x[tiles // 2 + t]
                mine_ref[at(j, 0), t * LANES : (t + 1) * LANES] = jnp.where(left, low, high)
                other_ref[at(j, 0), t * LANES : (t + 1) * LANES] = jnp.where(left, high, low)


VMEM = pl.BlockSpec(memory_space=pltpu.VMEM)


def near(*dims):
    return pltpu.VMEM(dims, F32)


def held(*values):
    return [pltpu.with_memory_space_constraint(v, pltpu.VMEM) for v in values]


def a_shape(level):
    return (6, TILES[level], 8 * STRIPS[level], LANES)


def v_shape(level):
    return (SOLVES[level] * TILES[level], BUF[level], LANES)


def c_shape(level):
    return (TILES[level], BUF[level], LANES)


FAR = pl.BlockSpec(memory_space=pltpu.HBM)


def call(kernel, arguments, outputs, scratch=(), aliases=None, sems=0, far=0):
    return pl.pallas_call(
        kernel,
        out_shape=outputs,
        in_specs=[FAR] * far + [VMEM] * (len(arguments) - far),
        out_specs=[FAR if isinstance(o, jax.ShapeDtypeStruct) else VMEM for o in outputs],
        scratch_shapes=[pltpu.VMEM(s, F32) for s in scratch] + ([pltpu.SemaphoreType.DMA((sems,))] if sems else []),
        input_output_aliases=aliases or {},
        compiler_params=pltpu.CompilerParams(vmem_limit_bytes=24 * 2**20),
        cost_estimate=pl.CostEstimate(flops=10**8, bytes_accessed=10**6, transcendentals=0),
    )(*arguments)


def swaps(distance):
    peers, samples = lax.axis_size("grid"), lax.axis_size("samp")
    even = [(i, i + distance if i % (2 * distance) < distance else i - distance) for i in range(peers)]
    odd = [(a + distance, b + distance) for a, b in even if max(a, b) + distance < peers]
    ends = sorted(set(range(peers)) - {a for a, _ in odd})
    both = [[(s * peers + a, s * peers + b) for s in range(samples) for a, b in pairs] for pairs in (even, odd)]
    both[1] += [(s * peers + e, (s + 1) % samples * peers + e) for s in range(samples) for e in ends]
    return both


def swapped(value, pairs):
    return lax.ppermute(value, ("samp", "grid"), pairs)


def gathered(value):
    sets = [pairs for distance in (1, 2) for pairs in swaps(distance)]
    return [swapped(value, pairs) for pairs in sets] + [value]


def local(log_coef, source):
    peers = lax.axis_size("grid")
    log_field, source_field = log_coef[0], source[0]
    rows, columns = source_field.shape
    far_fields = [pltpu.with_memory_space_constraint(x, pltpu.HBM) for x in (log_field, source_field)]
    tiled = [near(*c_shape(0)), near(*c_shape(0))]
    even, odd = swaps(1)
    edge = near(2 * TILES[0], NEAR, LANES)
    c0, s0, first, second, *fields = call(
        pack_kernel, far_fields, tiled + [edge, edge] + [near(rows, columns)] * 2, sems=6, far=2
    )
    near_rows = [swapped(first, even), swapped(second, odd)]
    edge = near(2 * TILES[0], HALO[0] - NEAR, LANES)
    c0, s0, first, second = call(pack_rest_kernel, held(*fields, c0, s0), tiled + [edge, edge], aliases={2: 0, 3: 1})
    rest_rows = [swapped(first, even), swapped(second, odd)]
    state = [near(*f(level)) for level in (0, 1) for f in (a_shape, v_shape, v_shape)]
    whole = tiled + state[:3] + [near(*c_shape(1))]
    started = call(functools.partial(inner_kernel, peers), held(*fields, c0, s0), whole, aliases={2: 0, 3: 1})
    *opened, message = call(
        functools.partial(open_kernel, peers), held(*started, *near_rows),
        whole + state[3:] + [near(3 * TILES[2], OWN[2], LANES)],
        [v_shape(0), v_shape(1)], {k: k for k in range(6)},
    )
    arrived = gathered(message)
    c0, s0, a0, b0, v0, _, a1, b1, v1 = call(
        functools.partial(outer_kernel, peers), held(*opened, *rest_rows),
        whole + state[3:], [v_shape(0)], {k: k for k in range(9)},
    )
    deep = [shape for level in (2, 3, 4) for shape in [c_shape(level)] + [v_shape(level)] * 3]
    message, a2, a3, a4, v0, b1, v1 = call(
        functools.partial(middle_kernel, peers),
        held(*arrived, a0, b0, v0, a1, b1, v1),
        [near(2 * TILES[2], OWN[2], LANES)] + [near(*a_shape(level)) for level in (2, 3, 4)] + [state[k] for k in (2, 4, 5)],
        [v_shape(0), v_shape(1)] + deep,
        {7: 4, 9: 5, 10: 6},
    )
    deep = [shape for level in (2, 3, 4) for shape in [v_shape(level)] * 3]
    half = near(rows, columns // 2)
    v0, v1, correction, mine, other = call(
        close_kernel,
        held(*gathered(message), a0, b0, v0, a1, b1, v1, a2, a3, a4),
        (state[2], state[5], near(rows, columns), half, half),
        [v_shape(0), v_shape(1)] + deep,
        {7: 0, 10: 1},
    )

    theirs = lax.ppermute(other, "samp", [(0, 1), (1, 0)])
    samples = lax.axis_size("samp")
    level_mean = (mine + theirs) / samples
    squares = mine * mine + theirs * theirs
    level_var = (squares - samples * level_mean * level_mean) / (samples - 1)
    return (correction[None], level_mean, level_var)


def solution(mesh):
    in_specs = (P("samp", "grid", None), P("samp", "grid", None))
    out_specs = (P("samp", "grid", None), P("grid", "samp"), P("grid", "samp"))
    return jax.shard_map(local, mesh=mesh, in_specs=in_specs, out_specs=out_specs, check_vma=False)
```
